32 devices in a mesh: dev: 32 (over z, y, x, core).
Axes of the slice: x: 2, y: 2, z: 4, core: 2. Of those that a mesh axis runs over, the one named last changes fastest.
Arguments:
- state: float32 [2, 1048576], P(None, 'dev'), as said below
- angles: float32 [20, 3], replicated, may hold values from -3.140625 to 3.140625
- sample_high: int32 [262144, 1], P('dev'), may hold values from 0 to 31; in each aligned block of 8192 rows (0 to 8191, 8192 to 16383, ...) at most 1024 rows name the same one
- sample_low: int32 [262144], P('dev'), may hold values from 0 to 32767
- marginal_qubits: int32 [10], replicated, may hold values from 0 to 19, as said below
Outputs:
- sample_probs: float32 [262144], P('dev')
- histogram: float32 [1024], P('dev')
- fidelity: float32 [], replicated
The draws below stay inside these ranges and needn't reach their ends.
Inputs may be any that keep to these rules, and one draw needn't show every extreme that they name: The state is unit noise times a product over qubits of factors between exp(-0.2) and exp(0.2). `marginal_qubits`: 10 different qubit numbers. `sample_high`: among the rows of one device no value occurs more than 1024 times, and in some devices one value occurs exactly 1024 times.
All inputs are finite; a program needn't handle non-finite values.
Results may differ from the reference program's by a relative error of at most 0.00075.
Values sent between devices are 32-bit elements.
A program may use at most 64 MiB of HBM per device.

```python
import math
import jax
import jax.numpy as jnp
import numpy as np

QUBITS = 20
AMPS_DEV = 32768
AMPS = 1048576
SAMP_DEV = 8192
SAMPLES = 262144
OWNERS = 32
CAP = 1024
MARG = 10
MARG_BINS = 1024


def draw_state(key, part):
    key_envelope = jax.random.fold_in(key, 11)
    key_noise = jax.random.fold_in(key, 12)
    factors = jax.random.uniform(key_envelope, (QUBITS,), jnp.float32, -0.15, 0.15)
    noise = jax.random.normal(key_noise, (2, AMPS), jnp.float32)
    index = jnp.arange(AMPS, dtype=jnp.int32)
    exponent = jnp.zeros((AMPS,), jnp.float32)
    for qubit in range(QUBITS):
        exponent = exponent + factors[qubit] * (index >> qubit & 1).astype(jnp.float32)
    return noise * jnp.exp(exponent)[None, :]


def draw_marginal_qubits(key, part):
    return jax.random.permutation(jax.random.fold_in(key, 21), QUBITS)[:MARG].astype(jnp.int32)


def set_ends(values, rng, least, top_value):
    spot = [jax.random.randint(jax.random.fold_in(rng, axis), (), 0, length) for axis, length in enumerate(values.shape)]
    widest = values.shape.index(max(values.shape))
    neighbour = spot[:widest] + [(spot[widest] + 1) % values.shape[widest]] + spot[widest + 1:]
    return values.at[tuple(spot)].set(least).at[tuple(neighbour)].set(top_value)


def rank_bounds(amount, lean):
    loads = [(1 << 20) // math.isqrt(standing ** lean) + 1 for standing in range(1, amount + 1)]
    deviation = 1 + sum(loads) // (1 << 30)
    return np.cumsum(np.array([max(1, weight // deviation) for weight in loads]))


def ranked_ids(stream_key, shape, number_of, skew):
    grid = rank_bounds(number_of, skew)
    pick = jax.random.randint(jax.random.fold_in(stream_key, 1), shape, 0, int(grid[number_of - 1]))
    standing = jnp.searchsorted(jnp.asarray(grid, jnp.int32), pick, side="right")
    return jax.random.permutation(jax.random.fold_in(stream_key, 2), number_of)[standing].astype(jnp.int32)


def assign_block(stream_key, own, number, rows, count, top, bound, skew):
    ranking = jax.random.permutation(stream_key, count)
    heavy_load, ordinary = portions_of(count, rows * top, bound, skew, True), portions_of(count, rows * top, bound, skew, False)
    places = jnp.arange(count)

    def named(lengths, offset_by):
        used = int((lengths > 0).sum())
        fixed = max(1, used // 4)
        passed = fixed + (places - fixed + offset_by * (used - fixed)) % max(1, count - fixed)
        return jnp.zeros((count,), jnp.int32).at[ranking[jnp.where(places < fixed, places, passed)]].set(jnp.asarray(lengths, jnp.int32))

    lengths = jnp.where(number % 4 == 0, named(heavy_load, number // 4), named(ordinary, number - number // 4 - 1))
    mixed = jax.random.permutation(jax.random.fold_in(own, 3), count)
    source_of, taker = mixed[0:count // 2 * 2:2], mixed[1:count // 2 * 2:2]
    margin = jnp.minimum(lengths[source_of] - 1, bound - lengths[taker]) // 2
    margin = jnp.where((source_of == ranking[0]) | (taker == ranking[0]) | (lengths[taker] == 0), 0, jnp.maximum(margin, 0))
    passed = jax.random.randint(jax.random.fold_in(own, 4), (count // 2,), 0, 1 << 20) % (margin + 1)
    lengths = lengths.at[source_of].add(-passed).at[taker].add(passed)
    items = jnp.searchsorted(jnp.cumsum(lengths), jnp.arange(rows * top), side="right").astype(jnp.int32)
    grid = items.reshape(top, rows).T
    grid = grid[jax.random.permutation(jax.random.fold_in(own, 1), rows)]
    offset_by = jax.random.randint(jax.random.fold_in(own, 2), (rows, 1), 0, top)
    return jnp.take_along_axis(grid, (jnp.arange(top)[None, :] + offset_by) % top, axis=1)


def portions_of(count, total, bound, skew, full):
    loads = [(1 << 20) // math.isqrt(grade ** skew) + 1 for grade in range(1, count + 1)]
    largest = bound if full else min(bound, max(-(-total // count), total * loads[0] // sum(loads)))
    least = 1 if total - largest >= count - 1 else 0
    counts, spare = [largest] + [least] * (count - 1), total - largest - least * (count - 1)
    while spare > 0:
        candidates = [i for i in range(1, count) if counts[i] < largest] or [i for i in range(1, count) if counts[i] < bound]
        whole, left = sum([loads[i] for i in candidates]), spare
        for i in candidates:
            more = min(bound - counts[i], max(1, left * loads[i] // whole), spare)
            counts[i] = counts[i] + more
            spare = spare - more
    return np.array(counts)


def setup_inputs(seed: int = 0) -> dict:
    keys = jax.random.split(jax.random.key(seed), 6)
    state = draw_state(jax.random.fold_in(keys[5], 71), 0)
    angles = jnp.clip(jax.random.uniform(keys[1], (QUBITS, 3), jnp.float32, -3.140625, 3.140625), -3.140625, 3.140625)
    sample_high_keys = jax.random.split(jax.random.fold_in(keys[2], 1), SAMPLES // SAMP_DEV)
    sample_high_turns = jax.random.permutation(jax.random.fold_in(keys[2], 3), SAMPLES // SAMP_DEV)
    sample_high = jax.vmap(lambda own, number: assign_block(jax.random.fold_in(keys[2], 2), own, number, SAMP_DEV, OWNERS, 1, CAP, 2))(sample_high_keys, sample_high_turns).reshape((SAMPLES, 1))
    sample_low = set_ends(ranked_ids(keys[3], (SAMPLES,), AMPS_DEV, 2), jax.random.fold_in(keys[3], 3), 0, AMPS_DEV - 1).astype(jnp.int32)
    marginal_qubits = draw_marginal_qubits(jax.random.fold_in(keys[5], 71), 0)
    return {"state": state, "angles": angles, "sample_high": sample_high, "sample_low": sample_low, "marginal_qubits": marginal_qubits}


def gate_parts(angles):
    theta = angles[:, 0]
    first = angles[:, 1]
    second = angles[:, 2]
    cosine = jnp.cos(theta)
    sine = jnp.sin(theta)
    zeros = jnp.zeros_like(cosine)
    real_part = jnp.stack([jnp.stack([cosine, -jnp.cos(second) * sine], -1),
                           jnp.stack([jnp.cos(first) * sine, jnp.cos(first + second) * cosine], -1)], -2)
    imag_part = jnp.stack([jnp.stack([zeros, -jnp.sin(second) * sine], -1),
                           jnp.stack([jnp.sin(first) * sine, jnp.sin(first + second) * cosine], -1)], -2)
    return real_part, imag_part


def reference(state, angles, sample_high, sample_low, marginal_qubits):
    gate_real, gate_imag = gate_parts(angles)
    real_part = state[0]
    imag_part = state[1]
    for qubit in range(QUBITS):
        shape = (AMPS // (2 * 2 ** qubit), 2, 2 ** qubit)
        field_real = real_part.reshape(shape)
        field_imag = imag_part.reshape(shape)
        zero_real, zero_imag = field_real[:, 0], field_imag[:, 0]
        one_real, one_imag = field_real[:, 1], field_imag[:, 1]
        outputs_real = []
        outputs_imag = []
        for row in range(2):
            ar, ai = gate_real[qubit, row, 0], gate_imag[qubit, row, 0]
            br, bi = gate_real[qubit, row, 1], gate_imag[qubit, row, 1]
            outputs_real.append(ar * zero_real - ai * zero_imag + br * one_real - bi * one_imag)
            outputs_imag.append(ar * zero_imag + ai * zero_real + br * one_imag + bi * one_real)
        real_part = jnp.stack(outputs_real, 1).reshape(AMPS)
        imag_part = jnp.stack(outputs_imag, 1).reshape(AMPS)
    weight = real_part * real_part + imag_part * imag_part
    norm = jnp.sum(weight)
    bitstring = sample_high[:, 0] * AMPS_DEV + sample_low
    sample_probs = AMPS * (jnp.take(weight, bitstring) / norm)
    fidelity = jnp.mean(sample_probs) - 1.0
    index = jnp.arange(AMPS, dtype=jnp.int32)
    bins = jnp.zeros((AMPS,), jnp.int32)
    for place in range(MARG):
        bins = bins + (((index >> marginal_qubits[place]) & 1) << place)
    totals = jax.ops.segment_sum(weight, bins, num_segments=MARG_BINS)
    histogram = MARG_BINS * (totals / norm)
    return sample_probs, histogram, fidelity
```

```python
import functools

import jax
import jax.numpy as jnp
from jax import lax
from jax.experimental import pallas as pl
from jax.experimental.pallas import tpu as pltpu
from jax.sharding import PartitionSpec as P

LANES = 128
SUBLANES = 8
f32 = jnp.float32
bf16 = jnp.bfloat16
i32 = jnp.int32


def gate_table(angles):
    entry = jnp.arange(8, dtype=i32)[None, :]
    cell = entry >> 1
    theta, first, second = angles[:, 0:1], angles[:, 1:2], angles[:, 2:3]
    phase = jnp.where(cell >= 2, first, 0.0) + jnp.where((cell & 1) == 1, second, 0.0)
    size = jnp.where((cell == 0) | (cell == 3), jnp.cos(theta), jnp.sin(theta))
    turn = jnp.where((entry & 1) == 0, jnp.cos(phase), jnp.sin(phase))
    return jnp.where(cell == 1, -1.0, 1.0) * size * turn


def iota(shape, dim):
    return lax.broadcasted_iota(i32, shape, dim)


def leading_gate(xr, xi, bit, u):
    n, s, lanes = xr.shape
    shape = (n >> (bit + 1), 2, 1 << bit, s, lanes)
    xr, xi = xr.reshape(shape), xi.reshape(shape)
    ar, ai, br, bi = xr[:, 0], xi[:, 0], xr[:, 1], xi[:, 1]
    outs_r, outs_i = [], []
    for row in range(2):
        pr, pi, qr, qi = u[4 * row : 4 * row + 4]
        outs_r.append(pr * ar - pi * ai + (qr * br - qi * bi))
        outs_i.append(pr * ai + pi * ar + (qr * bi + qi * br))
    return (
        jnp.stack(outs_r, 1).reshape(n, s, lanes),
        jnp.stack(outs_i, 1).reshape(n, s, lanes),
    )


def sublane_gate(xr, xi, bit, u):
    step = 1 << bit
    high = ((iota((SUBLANES, LANES), 0) >> bit) & 1) == 1

    def swap(x):
        down = pltpu.roll(x, step, 1)
        if 2 * step == SUBLANES:
            return down
        return jnp.where(high[None], down, pltpu.roll(x, SUBLANES - step, 1))

    keep_r = jnp.where(high, u[6], u[0])[None]
    keep_i = jnp.where(high, u[7], u[1])[None]
    cross_r = jnp.where(high, u[4], u[2])[None]
    cross_i = jnp.where(high, u[5], u[3])[None]
    yr, yi = swap(xr), swap(xi)
    return (
        keep_r * xr - keep_i * xi + (cross_r * yr - cross_i * yi),
        keep_r * xi + keep_i * xr + (cross_r * yi + cross_i * yr),
    )


def lane_matrix(units):
    shape = (LANES, LANES)
    row, col = iota(shape, 0), iota(shape, 1)
    mr = mi = None
    for bit, u in enumerate(units):
        rb, cb = ((row >> bit) & 1) == 1, ((col >> bit) & 1) == 1
        gr = jnp.where(cb, jnp.where(rb, u[6], u[4]), jnp.where(rb, u[2], u[0]))
        gi = jnp.where(cb, jnp.where(rb, u[7], u[5]), jnp.where(rb, u[3], u[1]))
        if mr is None:
            mr, mi = gr, gi
        else:
            mr, mi = mr * gr - mi * gi, mr * gi + mi * gr
    return mr, mi


def cut(x, depth):
    rows = x.shape[0]
    x = x.reshape(rows // SUBLANES, SUBLANES, LANES)
    per = SUBLANES // depth
    if per == 1:
        return x
    parts = [x[:, k * depth : (k + 1) * depth] for k in range(per)]
    return jnp.stack(parts, 1).reshape(rows // depth, depth, LANES)


def join(x):
    n, depth, _ = x.shape
    per = SUBLANES // depth
    if per > 1:
        x = x.reshape(n // per, per, depth, LANES)
        x = jnp.concatenate([x[:, k] for k in range(per)], axis=1)
    return x.reshape(n * depth, LANES)


def halves(x):
    top = x.astype(bf16)
    return top, (x - top.astype(f32)).astype(bf16)


def one_hot(row, count):
    wide = jnp.broadcast_to(row.astype(f32), (16, LANES)).astype(bf16)
    ids = iota((count, LANES), 0).astype(f32).astype(bf16).reshape(count // 16, 16, LANES)
    hot = jnp.where(ids == wide[None], jnp.ones((), bf16), jnp.zeros((), bf16))
    return hot.reshape(count, LANES)


def split_table(table):
    flipped = table.T
    top, rest = halves(flipped)
    return jnp.concatenate([top, rest], axis=0)


def lookup(table, upper, lower):
    rows = upper.shape[0]
    count = table.shape[1]
    hot = jnp.concatenate([one_hot(upper[r : r + 1], count) for r in range(rows)], axis=1)
    both = jnp.dot(table, hot, preferred_element_type=f32)
    lane_ids = iota((LANES, LANES), 0)
    found = []
    for r in range(rows):
        part = slice(r * LANES, (r + 1) * LANES)
        value = both[:LANES, part] + both[LANES:, part]
        value = jnp.where(lane_ids == lower[r : r + 1], value, 0.0)
        found.append(jnp.sum(value, axis=0, keepdims=True))
    return jnp.concatenate(found, axis=0)


def kernel(
    sizes,
    gates,
    marg,
    state,
    owner_ref,
    low_ref,
    probs_ref,
    hist_ref,
    fid_ref,
    amp_out,
    amp_in,
    wt_out,
    wt_in,
    req_out,
    req_in,
    ans_out,
    ans_in,
    his_out,
    his_in,
    tot_out,
    tot_in,
    code_ref,
    rank_ref,
    table_ref,
    sends,
    recvs,
):
    devices, depth, capacity_rows, marg_count, amps_total, samples = sizes
    me = lax.axis_index("dev")
    global_bits = devices.bit_length() - 1
    rows = state.shape[1]
    row_bits = rows.bit_length() - 1
    local_bits = row_bits + 7
    codes = devices * capacity_rows

    def peer(k):
        return lax.rem(me + k, devices)

    def copy(channel, src, dst, target):
        return pltpu.make_async_remote_copy(
            src_ref=src,
            dst_ref=dst,
            send_sem=sends.at[channel],
            recv_sem=recvs.at[channel],
            device_id=(target,),
            device_id_type=pl.DeviceIdType.MESH,
        )

    def scatter(channel, out, into):
        @pl.loop(1, devices)
        def _(k):
            target = peer(k)
            copy(channel, out.at[target], into.at[me], target).start()

        into[me] = out[me]

    def spread(channel, out, into):
        @pl.loop(1, devices)
        def _(k):
            copy(channel, out.at[0], into.at[me], peer(k)).start()

        into[me] = out[0]

    def all_of(channel, into):
        many = into.at[pl.ds(0, devices - 1)]
        return copy(channel, many, many, peer(1))

    barrier = pltpu.get_barrier_semaphore()

    @pl.loop(1, devices)
    def _(k):
        pl.semaphore_signal(
            barrier, inc=1, device_id=(peer(k),), device_id_type=pl.DeviceIdType.MESH
        )

    def unit(qubit):
        return [gates[qubit, e] for e in range(8)]

    mr, mi = lane_matrix([unit(q) for q in range(7)])
    mixed = jnp.concatenate(
        [jnp.concatenate([mr, mi], axis=1), jnp.concatenate([-mi, mr], axis=1)], axis=0
    )
    both = jnp.concatenate([state[0], state[1]], axis=1)
    both = jnp.dot(both, mixed, precision=lax.Precision.HIGHEST, preferred_element_type=f32)
    xr = both[:, :LANES].reshape(rows // SUBLANES, SUBLANES, LANES)
    xi = both[:, LANES:].reshape(rows // SUBLANES, SUBLANES, LANES)
    for bit in range(3):
        xr, xi = sublane_gate(xr, xi, bit, unit(7 + bit))
    for bit in range(row_bits - 3):
        xr, xi = leading_gate(xr, xi, bit, unit(10 + bit))
    amp_out[:, 0] = cut(xr.reshape(rows, LANES), depth)
    amp_out[:, 1] = cut(xi.reshape(rows, LANES), depth)

    pl.semaphore_wait(barrier, devices - 1)
    scatter(0, amp_out, amp_in)

    samp_rows = owner_ref.shape[0]
    owner = owner_ref[...]
    owner_ids = iota((devices, LANES), 0)
    chunks = samp_rows // 2
    hot_rows = [(owner_ids == owner[r : r + 1]) for r in range(samp_rows)]
    pieces = [h.astype(f32).astype(bf16) for h in hot_rows]
    stacked = jnp.concatenate(
        [jnp.concatenate(pieces[2 * c : 2 * c + 2], axis=1) for c in range(chunks)], axis=0
    )
    tri_shape = (2 * LANES, 3 * LANES)
    tri_row, tri_col = iota(tri_shape, 0), iota(tri_shape, 1)
    tri = ((tri_row < tri_col) | (tri_col >= 2 * LANES)).astype(f32).astype(bf16)
    counts = jnp.dot(stacked, tri, preferred_element_type=f32)
    before = jnp.zeros((devices, LANES), f32)
    ranks = []
    for c in range(chunks):
        block = counts[c * devices : (c + 1) * devices]
        for h in range(2):
            spot = block[:, h * LANES : (h + 1) * LANES] + before
            mine = owner_ids == owner[2 * c + h : 2 * c + h + 1]
            ranks.append(jnp.sum(jnp.where(mine, spot, 0.0), axis=0, keepdims=True))
        before = before + block[:, 2 * LANES :]
    ranking = jnp.concatenate(ranks, axis=0).astype(i32)
    code_ref[...] = owner * capacity_rows + (ranking >> 7)
    rank_ref[...] = ranking & (LANES - 1)

    lane_ids = iota((LANES, LANES), 0)
    steps = samp_rows // SUBLANES

    def place(t, placed):
        window = pl.ds(pl.multiple_of(t * SUBLANES, SUBLANES), SUBLANES)
        code, rank, low = code_ref[window], rank_ref[window], low_ref[window] + 1
        low_top = (low >> 8).astype(f32)
        low_rest = (low & 255).astype(f32)
        hot = jnp.concatenate([one_hot(code[r : r + 1], codes) for r in range(SUBLANES)], axis=1)
        tops, rests = [], []
        for r in range(SUBLANES):
            here = lane_ids == rank[r : r + 1]
            tops.append(jnp.where(here, low_top[r : r + 1], 0.0).astype(bf16))
            rests.append(jnp.where(here, low_rest[r : r + 1], 0.0).astype(bf16))
        values = jnp.concatenate(
            [jnp.concatenate(tops, axis=1), jnp.concatenate(rests, axis=1)], axis=0
        )
        return placed + lax.dot_general(
            hot, values, (((1,), (1,)), ((), ())), preferred_element_type=f32
        )

    placed = lax.fori_loop(0, steps, place, jnp.zeros((codes, 2 * LANES), f32))
    wanted = (placed[:, :LANES] * 256.0 + placed[:, LANES:]).astype(i32) - 1
    req_out[...] = cut(wanted, capacity_rows)
    scatter(1, req_out, req_in)

    all_of(0, amp_in).wait_recv()
    xr, xi = amp_in[:, 0], amp_in[:, 1]
    for bit in range(global_bits):
        xr, xi = leading_gate(xr, xi, bit, unit(local_bits + bit))
    weight = xr * xr + xi * xi
    wt_out[...] = weight
    scatter(2, wt_out, wt_in)

    weight = join(weight)
    norm_part = jnp.sum(weight, axis=0, keepdims=True)
    low_depth = depth.bit_length() - 1
    code_shape = (rows, LANES)
    row_id = iota(code_shape, 0)
    row_value = (
        ((row_id >> low_depth) << local_bits)
        + (me << (7 + low_depth))
        + ((row_id & (depth - 1)) << 7)
    )
    lane_value = iota((LANES, LANES), 0)
    row_code = jnp.zeros(code_shape, i32)
    lane_code = jnp.zeros((LANES, LANES), i32)
    lane_mask = jnp.zeros((), i32)
    for k in range(marg_count):
        qubit = marg[0, k]
        row_code = row_code + (((row_value >> qubit) & 1) << k)
        lane_code = lane_code + (((lane_value >> qubit) & 1) << k)
        lane_mask = lane_mask + jnp.where(qubit < 7, 1 << k, 0)
    bins = 2**marg_count
    top, rest = halves(weight)
    split = jnp.concatenate([top, rest], axis=0)
    @pl.loop(0, bins // LANES)
    def _(c):
        bin_id = c * LANES + iota((1, LANES), 1)
        lane_part = bin_id & lane_mask
        lane_hot = (lane_code == lane_part).astype(f32).astype(bf16)
        folded = jnp.dot(split, lane_hot, preferred_element_type=f32)
        folded = folded[:rows] + folded[rows:]
        picked = jnp.where(row_code == bin_id - lane_part, folded, 0.0)
        his_out[0, pl.ds(c, 1)] = jnp.sum(picked, axis=0, keepdims=True)

    spread(4, his_out, his_in)

    all_of(1, req_in).wait_recv()
    all_of(2, wt_in).wait_recv()
    table_ref[...] = split_table(join(wt_in[...]))

    def answer(target):
        wanted = req_in[target]
        return lookup(table_ref[...], wanted >> 7, wanted & (LANES - 1))

    def reply(k, total):
        target = peer(k)
        found = answer(target)
        ans_out[target] = found
        copy(3, ans_out.at[target], ans_in.at[me], target).start()
        return total + jnp.sum(found, axis=0, keepdims=True)

    total = lax.fori_loop(1, devices, reply, jnp.zeros((1, LANES), f32))
    found = answer(me)
    ans_in[me] = found
    total = total + jnp.sum(found, axis=0, keepdims=True)
    tot_out[0, 0:1] = total
    tot_out[0, 1:2] = norm_part
    spread(5, tot_out, tot_in)

    all_of(3, ans_in).wait_recv()
    table_ref[...] = split_table(join(ans_in[...]))

    def fetch(t, carry):
        window = pl.ds(pl.multiple_of(t * SUBLANES, SUBLANES), SUBLANES)
        probs_ref[window] = lookup(table_ref[...], code_ref[window], rank_ref[window])
        return carry

    lax.fori_loop(0, steps, fetch, 0)
    all_of(5, tot_in).wait_recv()
    all_of(4, his_in).wait_recv()
    sums = jnp.sum(jnp.sum(tot_in[...], axis=0), axis=1, keepdims=True)
    total, norm = sums[0:1], sums[1:2]
    probs_ref[...] = amps_total * (probs_ref[...] / norm)
    hist_ref[...] = float(bins) * (jnp.sum(his_in[...], axis=0) / norm)
    fid = amps_total * (total / norm) / samples - 1.0
    fid_ref[...] = jnp.broadcast_to(fid, (1, LANES))

    for channel, into in enumerate((amp_in, req_in, wt_in, ans_in, his_in, tot_in)):
        all_of(channel, into).wait_send()


def shards(state, angles, sample_high, sample_low, marginal_qubits):
    devices = lax.axis_size("dev")
    position = lax.axis_index("dev")
    amps_local = state.shape[1]
    samp_local = sample_low.shape[0]
    marg_count = marginal_qubits.shape[0]
    bins = 2**marg_count
    depth = amps_local // devices // LANES
    capacity_rows = 4 * samp_local // devices // LANES
    rows = amps_local // LANES
    samp_rows = samp_local // LANES
    sizes = (
        devices,
        depth,
        capacity_rows,
        marg_count,
        float(amps_local * devices),
        float(samp_local * devices),
    )
    vmem = pl.BlockSpec(memory_space=pltpu.VMEM)
    smem = pl.BlockSpec(memory_space=pltpu.SMEM)
    codes = devices * capacity_rows
    bin_rows = bins // LANES
    probs, hist, fid = pl.pallas_call(
        functools.partial(kernel, sizes),
        out_shape=(
            jax.ShapeDtypeStruct((samp_rows, LANES), f32),
            jax.ShapeDtypeStruct((bin_rows, LANES), f32),
            jax.ShapeDtypeStruct((1, LANES), f32),
        ),
        in_specs=[smem, smem, vmem, vmem, vmem],
        out_specs=(vmem, vmem, vmem),
        scratch_shapes=[
            pltpu.VMEM((devices, 2, depth, LANES), f32),
            pltpu.VMEM((devices, 2, depth, LANES), f32),
            pltpu.VMEM((devices, depth, LANES), f32),
            pltpu.VMEM((devices, depth, LANES), f32),
            pltpu.VMEM((devices, capacity_rows, LANES), i32),
            pltpu.VMEM((devices, capacity_rows, LANES), i32),
            pltpu.VMEM((devices, capacity_rows, LANES), f32),
            pltpu.VMEM((devices, capacity_rows, LANES), f32),
            pltpu.VMEM((1, bin_rows, LANES), f32),
            pltpu.VMEM((devices, bin_rows, LANES), f32),
            pltpu.VMEM((1, 2, LANES), f32),
            pltpu.VMEM((devices, 2, LANES), f32),
            pltpu.VMEM((samp_rows, LANES), i32),
            pltpu.VMEM((samp_rows, LANES), i32),
            pltpu.VMEM((2 * LANES, max(rows, codes)), bf16),
            pltpu.SemaphoreType.DMA((6,)),
            pltpu.SemaphoreType.DMA((6,)),
        ],
        compiler_params=pltpu.CompilerParams(collective_id=0, has_side_effects=True),
        name="circuit",
    )(
        gate_table(angles),
        marginal_qubits.reshape(1, marg_count),
        state.reshape(2, rows, LANES),
        sample_high.reshape(samp_rows, LANES),
        sample_low.reshape(samp_rows, LANES),
    )
    per_device = bins // devices
    mine = lax.dynamic_slice_in_dim(hist.reshape(bins), position * per_device, per_device)
    return probs.reshape(samp_local), mine, fid[0, 0]


def solution(mesh):
    return jax.shard_map(
        shards,
        mesh=mesh,
        in_specs=(P(None, "dev"), P(), P("dev", None), P("dev"), P()),
        out_specs=(P("dev"), P("dev"), P()),
        check_vma=False,
    )
```

```python
import functools

import jax
import jax.numpy as jnp
from jax import lax
from jax.experimental import pallas as pl
from jax.experimental.pallas import tpu as pltpu
from jax.sharding import PartitionSpec as P

LANES = 128
SUBLANES = 8
f32 = jnp.float32
bf16 = jnp.bfloat16
i32 = jnp.int32


def iota(shape, dim):
    return lax.broadcasted_iota(i32, shape, dim)


def gate_rows(angles, qubits):
    sub = iota((SUBLANES, LANES), 0)

    def column(j):
        blocks = []
        for first in range(0, qubits, SUBLANES):
            block = jnp.zeros((SUBLANES, LANES), f32)
            for q in range(first, min(first + SUBLANES, qubits)):
                block = jnp.where(sub == q - first, angles[j, q], block)
            blocks.append(block)
        return jnp.concatenate(blocks, axis=0)

    theta, first, second = column(0), column(1), column(2)
    cosine, sine = jnp.cos(theta), jnp.sin(theta)
    joint = first + second
    return [
        cosine,
        jnp.zeros_like(cosine),
        -jnp.cos(second) * sine,
        -jnp.sin(second) * sine,
        jnp.cos(first) * sine,
        jnp.sin(first) * sine,
        jnp.cos(joint) * cosine,
        jnp.sin(joint) * cosine,
    ]


def leading_gate(xr, xi, bit, u):
    n, s, lanes = xr.shape
    shape = (n >> (bit + 1), 2, 1 << bit, s, lanes)
    xr, xi = xr.reshape(shape), xi.reshape(shape)
    ar, ai, br, bi = xr[:, 0], xi[:, 0], xr[:, 1], xi[:, 1]
    outs_r, outs_i = [], []
    for row in range(2):
        pr, pi, qr, qi = u[4 * row : 4 * row + 4]
        outs_r.append(pr * ar - pi * ai + (qr * br - qi * bi))
        outs_i.append(pr * ai + pi * ar + (qr * bi + qi * br))
    return (
        jnp.stack(outs_r, 1).reshape(n, s, lanes),
        jnp.stack(outs_i, 1).reshape(n, s, lanes),
    )


def sublane_gate(xr, xi, bit, u):
    step = 1 << bit
    high = ((iota((SUBLANES, LANES), 0) >> bit) & 1) == 1

    def swap(x):
        down = pltpu.roll(x, step, 1)
        if 2 * step == SUBLANES:
            return down
        return jnp.where(high[None], down, pltpu.roll(x, SUBLANES - step, 1))

    keep_r = jnp.where(high, u[6], u[0])[None]
    keep_i = jnp.where(high, u[7], u[1])[None]
    cross_r = jnp.where(high, u[4], u[2])[None]
    cross_i = jnp.where(high, u[5], u[3])[None]
    yr, yi = swap(xr), swap(xi)
    return (
        keep_r * xr - keep_i * xi + (cross_r * yr - cross_i * yi),
        keep_r * xi + keep_i * xr + (cross_r * yi + cross_i * yr),
    )


def lane_matrix(units):
    shape = (LANES, LANES)
    row, col = iota(shape, 0), iota(shape, 1)
    mr = mi = None
    for bit, u in enumerate(units):
        rb, cb = ((row >> bit) & 1) == 1, ((col >> bit) & 1) == 1
        gr = jnp.where(cb, jnp.where(rb, u[6], u[4]), jnp.where(rb, u[2], u[0]))
        gi = jnp.where(cb, jnp.where(rb, u[7], u[5]), jnp.where(rb, u[3], u[1]))
        if mr is None:
            mr, mi = gr, gi
        else:
            mr, mi = mr * gr - mi * gi, mr * gi + mi * gr
    return mr, mi


def cut(x, depth):
    rows = x.shape[0]
    x = x.reshape(rows // SUBLANES, SUBLANES, LANES)
    per = SUBLANES // depth
    if per == 1:
        return x
    parts = [x[:, k * depth : (k + 1) * depth] for k in range(per)]
    return jnp.stack(parts, 1).reshape(rows // depth, depth, LANES)


def join(x):
    n, depth, _ = x.shape
    per = SUBLANES // depth
    if per > 1:
        x = x.reshape(n // per, per, depth, LANES)
        x = jnp.concatenate([x[:, k] for k in range(per)], axis=1)
    return x.reshape(n * depth, LANES)


def halves(x):
    top = x.astype(bf16)
    return top, (x - top.astype(f32)).astype(bf16)


def one_hot(row, count):
    wide = jnp.broadcast_to(row.astype(f32), (16, LANES)).astype(bf16)
    ids = iota((count, LANES), 0).astype(f32).astype(bf16).reshape(count // 16, 16, LANES)
    hot = jnp.where(ids == wide[None], jnp.ones((), bf16), jnp.zeros((), bf16))
    return hot.reshape(count, LANES)


def split_table(table):
    flipped = table.T
    top, rest = halves(flipped)
    return jnp.concatenate([top, rest], axis=0)


def lookup(table, upper, lower):
    rows = upper.shape[0]
    count = table.shape[1]
    hot = jnp.concatenate([one_hot(upper[r : r + 1], count) for r in range(rows)], axis=1)
    both = jnp.dot(table, hot, preferred_element_type=f32)
    lane_ids = iota((LANES, LANES), 0)
    found = []
    for r in range(rows):
        part = slice(r * LANES, (r + 1) * LANES)
        value = both[:LANES, part] + both[LANES:, part]
        value = jnp.where(lane_ids == lower[r : r + 1], value, 0.0)
        found.append(jnp.sum(value, axis=0, keepdims=True))
    return jnp.concatenate(found, axis=0)


def kernel(
    sizes,
    angles,
    marg,
    state,
    owner_ref,
    low_ref,
    probs_ref,
    hist_ref,
    fid_ref,
    amp_out,
    amp_in,
    wt_out,
    wt_in,
    req_out,
    req_in,
    ans_out,
    ans_in,
    his_out,
    his_in,
    tot_out,
    tot_in,
    code_ref,
    rank_ref,
    table_ref,
    gates,
    sends,
    recvs,
    req_recvs,
):
    devices, depth, capacity_rows, marg_count, amps_total, samples = sizes
    me = lax.axis_index("dev")
    global_bits = devices.bit_length() - 1
    rows = state.shape[0] // 2
    row_bits = rows.bit_length() - 1
    local_bits = row_bits + 7
    codes = devices * capacity_rows

    def peer(k):
        return lax.rem(me + k, devices)

    def copy(channel, src, dst, target):
        return pltpu.make_async_remote_copy(
            src_ref=src,
            dst_ref=dst,
            send_sem=sends.at[channel],
            recv_sem=recvs.at[channel],
            device_id=(target,),
            device_id_type=pl.DeviceIdType.MESH,
        )

    def scatter(channel, out, into):
        @pl.loop(1, devices)
        def _(k):
            target = peer(k)
            copy(channel, out.at[target], into.at[me], target).start()

        into[me] = out[me]

    def spread(channel, out, into):
        @pl.loop(1, devices)
        def _(k):
            copy(channel, out.at[0], into.at[me], peer(k)).start()

        into[me] = out[0]

    def all_of(channel, into):
        many = into.at[pl.ds(0, devices - 1)]
        return copy(channel, many, many, peer(1))

    def ask(src, source, target):
        return pltpu.make_async_remote_copy(
            src_ref=src,
            dst_ref=req_in.at[source],
            send_sem=sends.at[1],
            recv_sem=req_recvs.at[source],
            device_id=(target,),
            device_id_type=pl.DeviceIdType.MESH,
        )

    barrier = pltpu.get_barrier_semaphore()

    @pl.loop(1, devices)
    def _(k):
        pl.semaphore_signal(
            barrier, inc=1, device_id=(peer(k),), device_id_type=pl.DeviceIdType.MESH
        )

    for e, entry in enumerate(gate_rows(angles, global_bits + local_bits)):
        gates[e] = entry

    def unit(qubit):
        return [gates[e, qubit : qubit + 1] for e in range(8)]

    mr, mi = lane_matrix([unit(q) for q in range(7)])
    mixed = jnp.concatenate(
        [jnp.concatenate([mr, mi], axis=1), jnp.concatenate([-mi, mr], axis=1)], axis=0
    )
    both = jnp.concatenate(
        [state[pl.ds(0, rows, stride=2)], state[pl.ds(1, rows, stride=2)]], axis=1
    )
    both = jnp.dot(both, mixed, precision=lax.Precision.HIGHEST, preferred_element_type=f32)
    xr = both[:, :LANES].reshape(rows // SUBLANES, SUBLANES, LANES)
    xi = both[:, LANES:].reshape(rows // SUBLANES, SUBLANES, LANES)
    for bit in range(3):
        xr, xi = sublane_gate(xr, xi, bit, unit(7 + bit))
    for bit in range(row_bits - 3):
        xr, xi = leading_gate(xr, xi, bit, unit(10 + bit))
    amp_out[:, 0] = cut(xr.reshape(rows, LANES), depth)
    amp_out[:, 1] = cut(xi.reshape(rows, LANES), depth)

    pl.semaphore_wait(barrier, devices - 1)
    scatter(0, amp_out, amp_in)

    samp_rows = owner_ref.shape[0]
    owner = owner_ref[...]
    owner_ids = iota((devices, LANES), 0)
    chunks = samp_rows // 2
    hot_rows = [(owner_ids == owner[r : r + 1]) for r in range(samp_rows)]
    pieces = [h.astype(f32).astype(bf16) for h in hot_rows]
    stacked = jnp.concatenate(
        [jnp.concatenate(pieces[2 * c : 2 * c + 2], axis=1) for c in range(chunks)], axis=0
    )
    tri_shape = (2 * LANES, 3 * LANES)
    tri_row, tri_col = iota(tri_shape, 0), iota(tri_shape, 1)
    tri = ((tri_row < tri_col) | (tri_col >= 2 * LANES)).astype(f32).astype(bf16)
    counts = jnp.dot(stacked, tri, preferred_element_type=f32)
    before = jnp.zeros((devices, LANES), f32)
    ranks = []
    for c in range(chunks):
        block = counts[c * devices : (c + 1) * devices]
        for h in range(2):
            spot = block[:, h * LANES : (h + 1) * LANES] + before
            mine = owner_ids == owner[2 * c + h : 2 * c + h + 1]
            ranks.append(jnp.sum(jnp.where(mine, spot, 0.0), axis=0, keepdims=True))
        before = before + block[:, 2 * LANES :]
    ranking = jnp.concatenate(ranks, axis=0).astype(i32)
    code_ref[...] = owner * capacity_rows + (ranking >> 7)
    rank_ref[...] = ranking & (LANES - 1)

    lane_ids = iota((LANES, LANES), 0)
    steps = samp_rows // SUBLANES

    def place(t, placed):
        window = pl.ds(pl.multiple_of(t * SUBLANES, SUBLANES), SUBLANES)
        code, rank, low = code_ref[window], rank_ref[window], low_ref[window] + 1
        low_top = (low >> 8).astype(f32)
        low_rest = (low & 255).astype(f32)
        hot = jnp.concatenate([one_hot(code[r : r + 1], codes) for r in range(SUBLANES)], axis=1)
        tops, rests = [], []
        for r in range(SUBLANES):
            here = lane_ids == rank[r : r + 1]
            tops.append(jnp.where(here, low_top[r : r + 1], 0.0).astype(bf16))
            rests.append(jnp.where(here, low_rest[r : r + 1], 0.0).astype(bf16))
        values = jnp.concatenate(
            [jnp.concatenate(tops, axis=1), jnp.concatenate(rests, axis=1)], axis=0
        )
        return placed + lax.dot_general(
            hot, values, (((1,), (1,)), ((), ())), preferred_element_type=f32
        )

    placed = lax.fori_loop(0, steps, place, jnp.zeros((codes, 2 * LANES), f32))
    wanted = (placed[:, :LANES] * 256.0 + placed[:, LANES:]).astype(i32) - 1
    req_out[...] = cut(wanted, capacity_rows)

    all_of(0, amp_in).wait_recv()
    xr, xi = amp_in[:, 0], amp_in[:, 1]
    for bit in range(global_bits):
        xr, xi = leading_gate(xr, xi, bit, unit(local_bits + bit))
    weight = xr * xr + xi * xi
    wt_out[...] = weight
    scatter(2, wt_out, wt_in)

    @pl.loop(1, devices)
    def _(k):
        target = peer(k)
        ask(req_out.at[target], me, target).start()

    weight = join(weight)
    norm_part = jnp.sum(weight, axis=0, keepdims=True)
    low_depth = depth.bit_length() - 1
    code_shape = (rows, LANES)
    row_id = iota(code_shape, 0)
    row_value = (
        ((row_id >> low_depth) << local_bits)
        + (me << (7 + low_depth))
        + ((row_id & (depth - 1)) << 7)
    )
    lane_value = iota((LANES, LANES), 0)
    row_code = jnp.zeros(code_shape, i32)
    lane_code = jnp.zeros((LANES, LANES), i32)
    lane_mask = jnp.zeros((), i32)
    for k in range(marg_count):
        qubit = marg[0, k]
        row_code = row_code + (((row_value >> qubit) & 1) << k)
        lane_code = lane_code + (((lane_value >> qubit) & 1) << k)
        lane_mask = lane_mask + jnp.where(qubit < 7, 1 << k, 0)
    bins = 2**marg_count
    top, rest = halves(weight)
    split = jnp.concatenate([top, rest], axis=0)
    @pl.loop(0, bins // LANES)
    def _(c):
        bin_id = c * LANES + iota((1, LANES), 1)
        lane_part = bin_id & lane_mask
        lane_hot = (lane_code == lane_part).astype(f32).astype(bf16)
        folded = jnp.dot(split, lane_hot, preferred_element_type=f32)
        folded = folded[:rows] + folded[rows:]
        picked = jnp.where(row_code == bin_id - lane_part, folded, 0.0)
        his_out[0, pl.ds(c, 1)] = jnp.sum(picked, axis=0, keepdims=True)


    all_of(2, wt_in).wait_recv()
    spread(4, his_out, his_in)
    table_ref[...] = split_table(join(wt_in[...]))

    def answer(wanted):
        return lookup(table_ref[...], wanted >> 7, wanted & (LANES - 1))

    found = answer(req_out[me])
    ans_in[me] = found

    def reply(k, total):
        source = peer(devices - k)
        ask(req_out.at[source], source, source).wait_recv()
        found = answer(req_in[source])
        ans_out[source] = found
        copy(3, ans_out.at[source], ans_in.at[me], source).start()
        return total + jnp.sum(found, axis=0, keepdims=True)

    total = lax.fori_loop(1, devices, reply, jnp.sum(found, axis=0, keepdims=True))
    tot_out[0, 0:1] = total
    tot_out[0, 1:2] = norm_part
    spread(5, tot_out, tot_in)

    all_of(3, ans_in).wait_recv()
    table_ref[...] = split_table(join(ans_in[...]))

    def fetch(t, carry):
        window = pl.ds(pl.multiple_of(t * SUBLANES, SUBLANES), SUBLANES)
        probs_ref[window] = lookup(table_ref[...], code_ref[window], rank_ref[window])
        return carry

    lax.fori_loop(0, steps, fetch, 0)
    all_of(5, tot_in).wait_recv()
    all_of(4, his_in).wait_recv()
    sums = jnp.sum(jnp.sum(tot_in[...], axis=0), axis=1, keepdims=True)
    total, norm = sums[0:1], sums[1:2]
    probs_ref[...] = amps_total * (probs_ref[...] / norm)
    hist_ref[...] = float(bins) * (jnp.sum(his_in[...], axis=0) / norm)
    fid = amps_total * (total / norm) / samples - 1.0
    fid_ref[...] = jnp.broadcast_to(fid, (1, LANES))

    for channel, into in enumerate((amp_in, req_in, wt_in, ans_in, his_in, tot_in)):
        all_of(channel, into).wait_send()


def shards(state, angles, sample_high, sample_low, marginal_qubits):
    devices = lax.axis_size("dev")
    position = lax.axis_index("dev")
    amps_local = state.shape[1]
    samp_local = sample_low.shape[0]
    marg_count = marginal_qubits.shape[0]
    bins = 2**marg_count
    depth = amps_local // devices // LANES
    capacity_rows = 4 * samp_local // devices // LANES
    rows = amps_local // LANES
    samp_rows = samp_local // LANES
    sizes = (
        devices,
        depth,
        capacity_rows,
        marg_count,
        float(amps_local * devices),
        float(samp_local * devices),
    )
    vmem = pl.BlockSpec(memory_space=pltpu.VMEM)
    smem = pl.BlockSpec(memory_space=pltpu.SMEM)
    codes = devices * capacity_rows
    bin_rows = bins // LANES
    probs, hist, fid = pl.pallas_call(
        functools.partial(kernel, sizes),
        out_shape=(
            jax.ShapeDtypeStruct((samp_rows, LANES), f32),
            jax.ShapeDtypeStruct((bin_rows, LANES), f32),
            jax.ShapeDtypeStruct((1, LANES), f32),
        ),
        in_specs=[smem, smem, vmem, vmem, vmem],
        out_specs=(vmem, vmem, vmem),
        scratch_shapes=[
            pltpu.VMEM((devices, 2, depth, LANES), f32),
            pltpu.VMEM((devices, 2, depth, LANES), f32),
            pltpu.VMEM((devices, depth, LANES), f32),
            pltpu.VMEM((devices, depth, LANES), f32),
            pltpu.VMEM((devices, capacity_rows, LANES), i32),
            pltpu.VMEM((devices, capacity_rows, LANES), i32),
            pltpu.VMEM((devices, capacity_rows, LANES), f32),
            pltpu.VMEM((devices, capacity_rows, LANES), f32),
            pltpu.VMEM((1, bin_rows, LANES), f32),
            pltpu.VMEM((devices, bin_rows, LANES), f32),
            pltpu.VMEM((1, 2, LANES), f32),
            pltpu.VMEM((devices, 2, LANES), f32),
            pltpu.VMEM((samp_rows, LANES), i32),
            pltpu.VMEM((samp_rows, LANES), i32),
            pltpu.VMEM((2 * LANES, max(rows, codes)), bf16),
            pltpu.VMEM((8, -(-angles.shape[0] // SUBLANES) * SUBLANES, LANES), f32),
            pltpu.SemaphoreType.DMA((6,)),
            pltpu.SemaphoreType.DMA((6,)),
            pltpu.SemaphoreType.DMA((devices,)),
        ],
        compiler_params=pltpu.CompilerParams(collective_id=0, has_side_effects=True),
        name="circuit",
    )(
        angles.T,
        marginal_qubits.reshape(1, marg_count),
        state.reshape(2, rows, LANES).transpose(1, 0, 2).reshape(2 * rows, LANES),
        sample_high.reshape(samp_rows, LANES),
        sample_low.reshape(samp_rows, LANES),
    )
    per_device = bins // devices
    mine = lax.dynamic_slice_in_dim(hist.reshape(bins), position * per_device, per_device)
    return probs.reshape(samp_local), mine, fid[0, 0]


def solution(mesh):
    return jax.shard_map(
        shards,
        mesh=mesh,
        in_specs=(P(None, "dev"), P(), P("dev", None), P("dev"), P()),
        out_specs=(P("dev"), P("dev"), P()),
        check_vma=False,
    )
```

```python
import functools

import jax
import jax.numpy as jnp
from jax import lax
from jax.experimental import pallas as pl
from jax.experimental.pallas import tpu as pltpu
from jax.sharding import PartitionSpec as P

LANES = 128
SUBLANES = 8
f32 = jnp.float32
bf16 = jnp.bfloat16
i32 = jnp.int32


def iota(shape, dim):
    return lax.broadcasted_iota(i32, shape, dim)


def gate_rows(angles, qubits):
    sub = iota((SUBLANES, LANES), 0)

    def column(j):
        blocks = []
        for first in range(0, qubits, SUBLANES):
            block = jnp.zeros((SUBLANES, LANES), f32)
            for q in range(first, min(first + SUBLANES, qubits)):
                block = jnp.where(sub == q - first, angles[j, q], block)
            blocks.append(block)
        return jnp.concatenate(blocks, axis=0)

    theta, first, second = column(0), column(1), column(2)
    cosine, sine = jnp.cos(theta), jnp.sin(theta)
    joint = first + second
    return [
        cosine,
        jnp.zeros_like(cosine),
        -jnp.cos(second) * sine,
        -jnp.sin(second) * sine,
        jnp.cos(first) * sine,
        jnp.sin(first) * sine,
        jnp.cos(joint) * cosine,
        jnp.sin(joint) * cosine,
    ]


def leading_gate(xr, xi, bit, u):
    n, s, lanes = xr.shape
    shape = (n >> (bit + 1), 2, 1 << bit, s, lanes)
    xr, xi = xr.reshape(shape), xi.reshape(shape)
    ar, ai, br, bi = xr[:, 0], xi[:, 0], xr[:, 1], xi[:, 1]
    outs_r, outs_i = [], []
    for row in range(2):
        pr, pi, qr, qi = u[4 * row : 4 * row + 4]
        outs_r.append(pr * ar - pi * ai + (qr * br - qi * bi))
        outs_i.append(pr * ai + pi * ar + (qr * bi + qi * br))
    return (
        jnp.stack(outs_r, 1).reshape(n, s, lanes),
        jnp.stack(outs_i, 1).reshape(n, s, lanes),
    )


def sublane_gate(xr, xi, bit, u):
    step = 1 << bit
    high = ((iota((SUBLANES, LANES), 0) >> bit) & 1) == 1

    def swap(x):
        down = pltpu.roll(x, step, 1)
        if 2 * step == SUBLANES:
            return down
        return jnp.where(high[None], down, pltpu.roll(x, SUBLANES - step, 1))

    keep_r = jnp.where(high, u[6], u[0])[None]
    keep_i = jnp.where(high, u[7], u[1])[None]
    cross_r = jnp.where(high, u[4], u[2])[None]
    cross_i = jnp.where(high, u[5], u[3])[None]
    yr, yi = swap(xr), swap(xi)
    return (
        keep_r * xr - keep_i * xi + (cross_r * yr - cross_i * yi),
        keep_r * xi + keep_i * xr + (cross_r * yi + cross_i * yr),
    )


def lane_matrix(units):
    shape = (LANES, LANES)
    row, col = iota(shape, 0), iota(shape, 1)
    mr = mi = None
    for bit, u in enumerate(units):
        rb, cb = ((row >> bit) & 1) == 1, ((col >> bit) & 1) == 1
        gr = jnp.where(cb, jnp.where(rb, u[6], u[4]), jnp.where(rb, u[2], u[0]))
        gi = jnp.where(cb, jnp.where(rb, u[7], u[5]), jnp.where(rb, u[3], u[1]))
        if mr is None:
            mr, mi = gr, gi
        else:
            mr, mi = mr * gr - mi * gi, mr * gi + mi * gr
    return mr, mi


def cut(x, depth):
    rows = x.shape[0]
    x = x.reshape(rows // SUBLANES, SUBLANES, LANES)
    per = SUBLANES // depth
    if per == 1:
        return x
    parts = [x[:, k * depth : (k + 1) * depth] for k in range(per)]
    return jnp.stack(parts, 1).reshape(rows // depth, depth, LANES)


def join(x):
    n, depth, _ = x.shape
    per = SUBLANES // depth
    if per > 1:
        x = x.reshape(n // per, per, depth, LANES)
        x = jnp.concatenate([x[:, k] for k in range(per)], axis=1)
    return x.reshape(n * depth, LANES)


def halves(x):
    top = x.astype(bf16)
    return top, (x - top.astype(f32)).astype(bf16)


def one_hot(row, count):
    wide = jnp.broadcast_to(row.astype(f32), (16, LANES)).astype(bf16)
    ids = iota((count, LANES), 0).astype(f32).astype(bf16).reshape(count // 16, 16, LANES)
    hot = jnp.where(ids == wide[None], jnp.ones((), bf16), jnp.zeros((), bf16))
    return hot.reshape(count, LANES)


def split_table(table):
    flipped = table.T
    top, rest = halves(flipped)
    return jnp.concatenate([top, rest], axis=0)


def lookup_dot(table, upper, lower):
    rows = upper.shape[0]
    count = table.shape[1]
    hot = jnp.concatenate([one_hot(upper[r : r + 1], count) for r in range(rows)], axis=1)
    both = jnp.dot(table, hot, preferred_element_type=f32)
    lane_ids = iota((LANES, LANES), 0)
    found = []
    for r in range(rows):
        part = slice(r * LANES, (r + 1) * LANES)
        value = both[:LANES, part] + both[LANES:, part]
        value = jnp.where(lane_ids == lower[r : r + 1], value, 0.0)
        found.append(jnp.sum(value, axis=0, keepdims=True))
    return jnp.concatenate(found, axis=0)


def lookup_lanes(table_ref, upper, lower):
    rows = upper.shape[0]
    if rows < SUBLANES:
        upper = jnp.concatenate([upper] * (SUBLANES // rows), axis=0)
        lower = jnp.concatenate([lower] * (SUBLANES // rows), axis=0)
    shape = (SUBLANES, LANES)
    bits = table_ref.shape[0].bit_length() - 1
    high = [((upper >> bit) & 1) == 1 for bit in range(bits)]

    def pick(first, bit):
        if bit < 0:
            line = jnp.broadcast_to(table_ref[first : first + 1], shape)
            return jnp.take_along_axis(line, lower, axis=1, mode="promise_in_bounds")
        zero = pick(first, bit - 1)
        return jnp.where(high[bit], pick(first + (1 << bit), bit - 1), zero)

    return pick(0, bits - 1)[:rows]


def lookup_both(table, plain, wanted, other):
    one = lookup_dot(table, wanted[0], wanted[1])
    return one, lookup_lanes(plain, other[0], other[1])


def kernel(
    sizes,
    angles,
    marg,
    state,
    owner_ref,
    low_ref,
    probs_ref,
    hist_ref,
    fid_ref,
    amp_out,
    amp_in,
    wt_out,
    wt_in,
    req_out,
    req_in,
    ans_out,
    ans_in,
    his_out,
    his_in,
    tot_out,
    tot_in,
    code_ref,
    rank_ref,
    table_ref,
    plain_ref,
    back_ref,
    gates,
    sends,
    recvs,
    req_recvs,
):
    devices, depth, capacity_rows, marg_count, amps_total, samples = sizes
    me = lax.axis_index("dev")
    global_bits = devices.bit_length() - 1
    rows = state.shape[0] // 2
    row_bits = rows.bit_length() - 1
    local_bits = row_bits + 7
    codes = devices * capacity_rows

    def peer(k):
        return lax.rem(me + k, devices)

    def copy(channel, src, dst, target):
        return pltpu.make_async_remote_copy(
            src_ref=src,
            dst_ref=dst,
            send_sem=sends.at[channel],
            recv_sem=recvs.at[channel],
            device_id=(target,),
            device_id_type=pl.DeviceIdType.MESH,
        )

    def scatter(channel, out, into):
        @pl.loop(1, devices)
        def _(k):
            target = peer(k)
            copy(channel, out.at[target], into.at[me], target).start()

        into[me] = out[me]

    def spread(channel, out, into):
        @pl.loop(1, devices)
        def _(k):
            copy(channel, out.at[0], into.at[me], peer(k)).start()

        into[me] = out[0]

    def all_of(channel, into):
        many = into.at[pl.ds(0, devices - 1)]
        return copy(channel, many, many, peer(1))

    def ask(src, source, target):
        return pltpu.make_async_remote_copy(
            src_ref=src,
            dst_ref=req_in.at[source],
            send_sem=sends.at[1],
            recv_sem=req_recvs.at[source],
            device_id=(target,),
            device_id_type=pl.DeviceIdType.MESH,
        )

    barrier = pltpu.get_barrier_semaphore()

    @pl.loop(1, devices)
    def _(k):
        pl.semaphore_signal(
            barrier, inc=1, device_id=(peer(k),), device_id_type=pl.DeviceIdType.MESH
        )

    for e, entry in enumerate(gate_rows(angles, global_bits + local_bits)):
        gates[e] = entry

    def unit(qubit):
        return [gates[e, qubit : qubit + 1] for e in range(8)]

    mr, mi = lane_matrix([unit(q) for q in range(7)])
    mixed = jnp.concatenate(
        [jnp.concatenate([mr, mi], axis=1), jnp.concatenate([-mi, mr], axis=1)], axis=0
    )
    both = jnp.concatenate(
        [state[pl.ds(0, rows, stride=2)], state[pl.ds(1, rows, stride=2)]], axis=1
    )
    both = jnp.dot(both, mixed, precision=lax.Precision.HIGHEST, preferred_element_type=f32)
    xr = both[:, :LANES].reshape(rows // SUBLANES, SUBLANES, LANES)
    xi = both[:, LANES:].reshape(rows // SUBLANES, SUBLANES, LANES)
    for bit in range(3):
        xr, xi = sublane_gate(xr, xi, bit, unit(7 + bit))
    for bit in range(row_bits - 3):
        xr, xi = leading_gate(xr, xi, bit, unit(10 + bit))
    amp_out[:, 0] = cut(xr.reshape(rows, LANES), depth)
    amp_out[:, 1] = cut(xi.reshape(rows, LANES), depth)

    pl.semaphore_wait(barrier, devices - 1)
    scatter(0, amp_out, amp_in)

    samp_rows = owner_ref.shape[0]
    owner = owner_ref[...]
    owner_ids = iota((devices, LANES), 0)
    chunks = samp_rows // 2
    hot_rows = [(owner_ids == owner[r : r + 1]) for r in range(samp_rows)]
    pieces = [h.astype(f32).astype(bf16) for h in hot_rows]
    stacked = jnp.concatenate(
        [jnp.concatenate(pieces[2 * c : 2 * c + 2], axis=1) for c in range(chunks)], axis=0
    )
    tri_shape = (2 * LANES, 3 * LANES)
    tri_row, tri_col = iota(tri_shape, 0), iota(tri_shape, 1)
    tri = ((tri_row < tri_col) | (tri_col >= 2 * LANES)).astype(f32).astype(bf16)
    counts = jnp.dot(stacked, tri, preferred_element_type=f32)
    before = jnp.zeros((devices, LANES), f32)
    ranks = []
    for c in range(chunks):
        block = counts[c * devices : (c + 1) * devices]
        for h in range(2):
            spot = block[:, h * LANES : (h + 1) * LANES] + before
            mine = owner_ids == owner[2 * c + h : 2 * c + h + 1]
            ranks.append(jnp.sum(jnp.where(mine, spot, 0.0), axis=0, keepdims=True))
        before = before + block[:, 2 * LANES :]
    ranking = jnp.concatenate(ranks, axis=0).astype(i32)
    code_ref[...] = owner * capacity_rows + (ranking >> 7)
    rank_ref[...] = ranking & (LANES - 1)

    lane_ids = iota((LANES, LANES), 0)
    steps = samp_rows // SUBLANES

    def place(t, placed):
        window = pl.ds(pl.multiple_of(t * SUBLANES, SUBLANES), SUBLANES)
        code, rank, low = code_ref[window], rank_ref[window], low_ref[window] + 1
        low_top = (low >> 8).astype(f32)
        low_rest = (low & 255).astype(f32)
        hot = jnp.concatenate([one_hot(code[r : r + 1], codes) for r in range(SUBLANES)], axis=1)
        tops, rests = [], []
        for r in range(SUBLANES):
            here = lane_ids == rank[r : r + 1]
            tops.append(jnp.where(here, low_top[r : r + 1], 0.0).astype(bf16))
            rests.append(jnp.where(here, low_rest[r : r + 1], 0.0).astype(bf16))
        values = jnp.concatenate(
            [jnp.concatenate(tops, axis=1), jnp.concatenate(rests, axis=1)], axis=0
        )
        return placed + lax.dot_general(
            hot, values, (((1,), (1,)), ((), ())), preferred_element_type=f32
        )

    placed = lax.fori_loop(0, steps, place, jnp.zeros((codes, 2 * LANES), f32))
    wanted = (placed[:, :LANES] * 256.0 + placed[:, LANES:]).astype(i32) - 1
    req_out[...] = cut(wanted, capacity_rows)

    all_of(0, amp_in).wait_recv()
    xr, xi = amp_in[:, 0], amp_in[:, 1]
    for bit in range(global_bits):
        xr, xi = leading_gate(xr, xi, bit, unit(local_bits + bit))
    weight = xr * xr + xi * xi
    wt_out[...] = weight
    scatter(2, wt_out, wt_in)

    @pl.loop(1, devices)
    def _(k):
        target = peer(k)
        ask(req_out.at[target], me, target).start()

    weight = join(weight)
    norm_part = jnp.sum(weight, axis=0, keepdims=True)
    low_depth = depth.bit_length() - 1
    code_shape = (rows, LANES)
    row_id = iota(code_shape, 0)
    row_value = (
        ((row_id >> low_depth) << local_bits)
        + (me << (7 + low_depth))
        + ((row_id & (depth - 1)) << 7)
    )
    lane_value = iota((LANES, LANES), 0)
    row_code = jnp.zeros(code_shape, i32)
    lane_code = jnp.zeros((LANES, LANES), i32)
    lane_mask = jnp.zeros((), i32)
    for k in range(marg_count):
        qubit = marg[0, k]
        row_code = row_code + (((row_value >> qubit) & 1) << k)
        lane_code = lane_code + (((lane_value >> qubit) & 1) << k)
        lane_mask = lane_mask + jnp.where(qubit < 7, 1 << k, 0)
    bins = 2**marg_count
    top, rest = halves(weight)
    split = jnp.concatenate([top, rest], axis=0)
    @pl.loop(0, bins // LANES)
    def _(c):
        bin_id = c * LANES + iota((1, LANES), 1)
        lane_part = bin_id & lane_mask
        lane_hot = (lane_code == lane_part).astype(f32).astype(bf16)
        folded = jnp.dot(split, lane_hot, preferred_element_type=f32)
        folded = folded[:rows] + folded[rows:]
        picked = jnp.where(row_code == bin_id - lane_part, folded, 0.0)
        his_out[0, pl.ds(c, 1)] = jnp.sum(picked, axis=0, keepdims=True)


    all_of(2, wt_in).wait_recv()
    spread(4, his_out, his_in)
    plain_ref[...] = join(wt_in[...])
    table_ref[...] = split_table(plain_ref[...])

    def parts(wanted):
        return wanted >> 7, wanted & (LANES - 1)

    def answers(wanted, other):
        found, second = lookup_both(
            table_ref[:, 0:rows], plain_ref, parts(wanted), parts(other)
        )
        return found, jnp.where(other >= 0, second, 0.0)

    def asked(k):
        source = peer(devices - k)
        ask(req_out.at[source], source, source).wait_recv()
        return source

    def send(source, found):
        ans_out[source] = found
        copy(3, ans_out.at[source], ans_in.at[me], source).start()

    source = asked(1)
    found, own = answers(req_in[source], req_out[me])
    send(source, found)
    ans_in[me] = own

    def reply(t, total):
        first, second = asked(2 * t), asked(2 * t + 1)
        found, other = answers(req_in[first], req_in[second])
        send(first, found)
        send(second, other)
        return total + jnp.sum(found + other, axis=0, keepdims=True)

    total = jnp.sum(found + own, axis=0, keepdims=True)
    total = lax.fori_loop(1, devices // 2, reply, total)
    tot_out[0, 0:1] = total
    tot_out[0, 1:2] = norm_part
    spread(5, tot_out, tot_in)

    all_of(3, ans_in).wait_recv()
    back_ref[...] = join(ans_in[...])
    table_ref[:, 0:codes] = split_table(back_ref[...])

    def fetch(t, carry):
        one = pl.ds(pl.multiple_of(2 * t * SUBLANES, SUBLANES), SUBLANES)
        two = pl.ds(pl.multiple_of((2 * t + 1) * SUBLANES, SUBLANES), SUBLANES)
        probs_ref[one], probs_ref[two] = lookup_both(
            table_ref[:, 0:codes],
            back_ref,
            (code_ref[one], rank_ref[one]),
            (code_ref[two], rank_ref[two]),
        )
        return carry

    lax.fori_loop(0, steps // 2, fetch, 0)
    all_of(5, tot_in).wait_recv()
    all_of(4, his_in).wait_recv()
    sums = jnp.sum(jnp.sum(tot_in[...], axis=0), axis=1, keepdims=True)
    total, norm = sums[0:1], sums[1:2]
    probs_ref[...] = amps_total * (probs_ref[...] / norm)
    hist_ref[...] = float(bins) * (jnp.sum(his_in[...], axis=0) / norm)
    fid = amps_total * (total / norm) / samples - 1.0
    fid_ref[...] = jnp.broadcast_to(fid, (1, LANES))

    for channel, into in enumerate((amp_in, req_in, wt_in, ans_in, his_in, tot_in)):
        all_of(channel, into).wait_send()


def shards(state, angles, sample_high, sample_low, marginal_qubits):
    devices = lax.axis_size("dev")
    position = lax.axis_index("dev")
    amps_local = state.shape[1]
    samp_local = sample_low.shape[0]
    marg_count = marginal_qubits.shape[0]
    bins = 2**marg_count
    depth = amps_local // devices // LANES
    capacity_rows = 4 * samp_local // devices // LANES
    rows = amps_local // LANES
    samp_rows = samp_local // LANES
    sizes = (
        devices,
        depth,
        capacity_rows,
        marg_count,
        float(amps_local * devices),
        float(samp_local * devices),
    )
    vmem = pl.BlockSpec(memory_space=pltpu.VMEM)
    smem = pl.BlockSpec(memory_space=pltpu.SMEM)
    codes = devices * capacity_rows
    bin_rows = bins // LANES
    probs, hist, fid = pl.pallas_call(
        functools.partial(kernel, sizes),
        out_shape=(
            jax.ShapeDtypeStruct((samp_rows, LANES), f32),
            jax.ShapeDtypeStruct((bin_rows, LANES), f32),
            jax.ShapeDtypeStruct((1, LANES), f32),
        ),
        in_specs=[smem, smem, vmem, vmem, vmem],
        out_specs=(vmem, vmem, vmem),
        scratch_shapes=[
            pltpu.VMEM((devices, 2, depth, LANES), f32),
            pltpu.VMEM((devices, 2, depth, LANES), f32),
            pltpu.VMEM((devices, depth, LANES), f32),
            pltpu.VMEM((devices, depth, LANES), f32),
            pltpu.VMEM((devices, capacity_rows, LANES), i32),
            pltpu.VMEM((devices, capacity_rows, LANES), i32),
            pltpu.VMEM((devices, capacity_rows, LANES), f32),
            pltpu.VMEM((devices, capacity_rows, LANES), f32),
            pltpu.VMEM((1, bin_rows, LANES), f32),
            pltpu.VMEM((devices, bin_rows, LANES), f32),
            pltpu.VMEM((1, 2, LANES), f32),
            pltpu.VMEM((devices, 2, LANES), f32),
            pltpu.VMEM((samp_rows, LANES), i32),
            pltpu.VMEM((samp_rows, LANES), i32),
            pltpu.VMEM((2 * LANES, max(rows, codes)), bf16),
            pltpu.VMEM((rows, LANES), f32),
            pltpu.VMEM((codes, LANES), f32),
            pltpu.VMEM((8, -(-angles.shape[0] // SUBLANES) * SUBLANES, LANES), f32),
            pltpu.SemaphoreType.DMA((6,)),
            pltpu.SemaphoreType.DMA((6,)),
            pltpu.SemaphoreType.DMA((devices,)),
        ],
        compiler_params=pltpu.CompilerParams(collective_id=0, has_side_effects=True),
        name="circuit",
    )(
        angles.T,
        marginal_qubits.reshape(1, marg_count),
        state.reshape(2, rows, LANES).transpose(1, 0, 2).reshape(2 * rows, LANES),
        sample_high.reshape(samp_rows, LANES),
        sample_low.reshape(samp_rows, LANES),
    )
    per_device = bins // devices
    mine = lax.dynamic_slice_in_dim(hist.reshape(bins), position * per_device, per_device)
    return probs.reshape(samp_local), mine, fid[0, 0]


def solution(mesh):
    return jax.shard_map(
        shards,
        mesh=mesh,
        in_specs=(P(None, "dev"), P(), P("dev", None), P("dev"), P()),
        out_specs=(P("dev"), P("dev"), P()),
        check_vma=False,
    )
```

```python
import functools

import jax
import jax.numpy as jnp
from jax import lax
from jax.experimental import pallas as pl
from jax.experimental.pallas import tpu as pltpu
from jax.sharding import PartitionSpec as P

LANES = 128
SUBLANES = 8
f32 = jnp.float32
bf16 = jnp.bfloat16
i32 = jnp.int32


def iota(shape, dim):
    return lax.broadcasted_iota(i32, shape, dim)


def gate_rows(angles, qubits):
    sub = iota((SUBLANES, LANES), 0)

    def column(j):
        blocks = []
        for first in range(0, qubits, SUBLANES):
            block = jnp.zeros((SUBLANES, LANES), f32)
            for q in range(first, min(first + SUBLANES, qubits)):
                block = jnp.where(sub == q - first, angles[j, q], block)
            blocks.append(block)
        return jnp.concatenate(blocks, axis=0)

    theta, first, second = column(0), column(1), column(2)
    cosine, sine = jnp.cos(theta), jnp.sin(theta)
    joint = first + second
    return [
        cosine,
        jnp.zeros_like(cosine),
        -jnp.cos(second) * sine,
        -jnp.sin(second) * sine,
        jnp.cos(first) * sine,
        jnp.sin(first) * sine,
        jnp.cos(joint) * cosine,
        jnp.sin(joint) * cosine,
    ]


def leading_gate(xr, xi, bit, u):
    n, s, lanes = xr.shape
    shape = (n >> (bit + 1), 2, 1 << bit, s, lanes)
    xr, xi = xr.reshape(shape), xi.reshape(shape)
    ar, ai, br, bi = xr[:, 0], xi[:, 0], xr[:, 1], xi[:, 1]
    outs_r, outs_i = [], []
    for row in range(2):
        pr, pi, qr, qi = u[4 * row : 4 * row + 4]
        outs_r.append(pr * ar - pi * ai + (qr * br - qi * bi))
        outs_i.append(pr * ai + pi * ar + (qr * bi + qi * br))
    return (
        jnp.stack(outs_r, 1).reshape(n, s, lanes),
        jnp.stack(outs_i, 1).reshape(n, s, lanes),
    )


def sublane_gate(xr, xi, bit, u):
    step = 1 << bit
    high = ((iota((SUBLANES, LANES), 0) >> bit) & 1) == 1

    def swap(x):
        down = pltpu.roll(x, step, 1)
        if 2 * step == SUBLANES:
            return down
        return jnp.where(high[None], down, pltpu.roll(x, SUBLANES - step, 1))

    keep_r = jnp.where(high, u[6], u[0])[None]
    keep_i = jnp.where(high, u[7], u[1])[None]
    cross_r = jnp.where(high, u[4], u[2])[None]
    cross_i = jnp.where(high, u[5], u[3])[None]
    yr, yi = swap(xr), swap(xi)
    return (
        keep_r * xr - keep_i * xi + (cross_r * yr - cross_i * yi),
        keep_r * xi + keep_i * xr + (cross_r * yi + cross_i * yr),
    )


def lane_matrix(units):
    shape = (LANES, LANES)
    row, col = iota(shape, 0), iota(shape, 1)
    mr = mi = None
    for bit, u in enumerate(units):
        rb, cb = ((row >> bit) & 1) == 1, ((col >> bit) & 1) == 1
        gr = jnp.where(cb, jnp.where(rb, u[6], u[4]), jnp.where(rb, u[2], u[0]))
        gi = jnp.where(cb, jnp.where(rb, u[7], u[5]), jnp.where(rb, u[3], u[1]))
        if mr is None:
            mr, mi = gr, gi
        else:
            mr, mi = mr * gr - mi * gi, mr * gi + mi * gr
    return mr, mi


def cut(x, depth):
    rows = x.shape[0]
    x = x.reshape(rows // SUBLANES, SUBLANES, LANES)
    per = SUBLANES // depth
    if per == 1:
        return x
    parts = [x[:, k * depth : (k + 1) * depth] for k in range(per)]
    return jnp.stack(parts, 1).reshape(rows // depth, depth, LANES)


def join(x):
    n, depth, _ = x.shape
    per = SUBLANES // depth
    if per > 1:
        x = x.reshape(n // per, per, depth, LANES)
        x = jnp.concatenate([x[:, k] for k in range(per)], axis=1)
    return x.reshape(n * depth, LANES)


def halves(x):
    top = x.astype(bf16)
    return top, (x - top.astype(f32)).astype(bf16)


def one_hot(row, count):
    wide = jnp.broadcast_to(row.astype(f32), (16, LANES)).astype(bf16)
    ids = iota((count, LANES), 0).astype(f32).astype(bf16).reshape(count // 16, 16, LANES)
    hot = jnp.where(ids == wide[None], jnp.ones((), bf16), jnp.zeros((), bf16))
    return hot.reshape(count, LANES)


def split_table(table):
    flipped = table.T
    top, rest = halves(flipped)
    return jnp.concatenate([top, rest], axis=0)


def lookup_dot(table, upper, lower):
    rows = upper.shape[0]
    count = table.shape[1]
    hot = jnp.concatenate([one_hot(upper[r : r + 1], count) for r in range(rows)], axis=1)
    both = jnp.dot(table, hot, preferred_element_type=f32)
    lane_ids = iota((LANES, LANES), 0)
    found = []
    for r in range(rows):
        part = slice(r * LANES, (r + 1) * LANES)
        value = both[:LANES, part] + both[LANES:, part]
        value = jnp.where(lane_ids == lower[r : r + 1], value, 0.0)
        found.append(jnp.sum(value, axis=0, keepdims=True))
    return jnp.concatenate(found, axis=0)


def lookup_lanes(table_ref, upper, lower):
    rows = upper.shape[0]
    if rows < SUBLANES:
        upper = jnp.concatenate([upper] * (SUBLANES // rows), axis=0)
        lower = jnp.concatenate([lower] * (SUBLANES // rows), axis=0)
    shape = (SUBLANES, LANES)
    bits = table_ref.shape[0].bit_length() - 1
    high = [((upper >> bit) & 1) == 1 for bit in range(bits)]

    def pick(first, bit):
        if bit < 0:
            line = jnp.broadcast_to(table_ref[first : first + 1], shape)
            return jnp.take_along_axis(line, lower, axis=1, mode="promise_in_bounds")
        zero = pick(first, bit - 1)
        return jnp.where(high[bit], pick(first + (1 << bit), bit - 1), zero)

    return pick(0, bits - 1)[:rows]


def lookup_both(table, plain, wanted, other):
    one = lookup_dot(table, wanted[0], wanted[1])
    return one, lookup_lanes(plain, other[0], other[1])


def kernel(
    sizes,
    angles,
    marg,
    state,
    owner_ref,
    low_ref,
    probs_ref,
    hist_ref,
    fid_ref,
    amp_out,
    amp_in,
    wt_out,
    wt_in,
    req_out,
    req_in,
    ans_out,
    ans_in,
    his_out,
    his_in,
    tot_out,
    tot_in,
    code_ref,
    rank_ref,
    table_ref,
    plain_ref,
    back_ref,
    gates,
    sends,
    recvs,
    req_recvs,
):
    devices, depth, capacity_rows, marg_count = sizes
    me = lax.axis_index("dev")
    global_bits = devices.bit_length() - 1
    rows = state.shape[0] // 2
    row_bits = rows.bit_length() - 1
    local_bits = row_bits + 7
    codes = devices * capacity_rows

    def peer(k):
        return lax.rem(me + k, devices)

    def copy(channel, src, dst, target):
        return pltpu.make_async_remote_copy(
            src_ref=src,
            dst_ref=dst,
            send_sem=sends.at[channel],
            recv_sem=recvs.at[channel],
            device_id=(target,),
            device_id_type=pl.DeviceIdType.MESH,
        )

    def scatter(channel, out, into):
        @pl.loop(1, devices)
        def _(k):
            target = peer(k)
            copy(channel, out.at[target], into.at[me], target).start()

        into[me] = out[me]

    def spread(channel, out, into):
        @pl.loop(1, devices)
        def _(k):
            copy(channel, out.at[0], into.at[me], peer(k)).start()

        into[me] = out[0]

    def all_of(channel, into):
        many = into.at[pl.ds(0, devices - 1)]
        return copy(channel, many, many, peer(1))

    def ask(src, source, target):
        return pltpu.make_async_remote_copy(
            src_ref=src,
            dst_ref=req_in.at[source],
            send_sem=sends.at[1],
            recv_sem=req_recvs.at[source],
            device_id=(target,),
            device_id_type=pl.DeviceIdType.MESH,
        )

    barrier = pltpu.get_barrier_semaphore()

    @pl.loop(1, devices)
    def _(k):
        pl.semaphore_signal(
            barrier, inc=1, device_id=(peer(k),), device_id_type=pl.DeviceIdType.MESH
        )

    for e, entry in enumerate(gate_rows(angles, global_bits + local_bits)):
        gates[e] = entry

    def unit(qubit):
        return [gates[e, qubit : qubit + 1] for e in range(8)]

    mr, mi = lane_matrix([unit(q) for q in range(7)])
    mixed = jnp.concatenate(
        [jnp.concatenate([mr, mi], axis=1), jnp.concatenate([-mi, mr], axis=1)], axis=0
    )
    both = jnp.concatenate(
        [state[pl.ds(0, rows, stride=2)], state[pl.ds(1, rows, stride=2)]], axis=1
    )
    both = jnp.dot(both, mixed, precision=lax.Precision.HIGHEST, preferred_element_type=f32)
    xr = both[:, :LANES].reshape(rows // SUBLANES, SUBLANES, LANES)
    xi = both[:, LANES:].reshape(rows // SUBLANES, SUBLANES, LANES)
    for bit in range(3):
        xr, xi = sublane_gate(xr, xi, bit, unit(7 + bit))
    for bit in range(row_bits - 3):
        xr, xi = leading_gate(xr, xi, bit, unit(10 + bit))
    amp_out[:, 0] = cut(xr.reshape(rows, LANES), depth)
    amp_out[:, 1] = cut(xi.reshape(rows, LANES), depth)

    pl.semaphore_wait(barrier, devices - 1)
    scatter(0, amp_out, amp_in)

    samp_rows = owner_ref.shape[0]
    owner = owner_ref[...]
    owner_ids = iota((devices, LANES), 0)
    chunks = samp_rows // 2
    hot_rows = [(owner_ids == owner[r : r + 1]) for r in range(samp_rows)]
    pieces = [h.astype(f32).astype(bf16) for h in hot_rows]
    stacked = jnp.concatenate(
        [jnp.concatenate(pieces[2 * c : 2 * c + 2], axis=1) for c in range(chunks)], axis=0
    )
    tri_shape = (2 * LANES, 3 * LANES)
    tri_row, tri_col = iota(tri_shape, 0), iota(tri_shape, 1)
    tri = ((tri_row < tri_col) | (tri_col >= 2 * LANES)).astype(f32).astype(bf16)
    counts = jnp.dot(stacked, tri, preferred_element_type=f32)
    before = jnp.zeros((devices, LANES), f32)
    ranks = []
    for c in range(chunks):
        block = counts[c * devices : (c + 1) * devices]
        for h in range(2):
            spot = block[:, h * LANES : (h + 1) * LANES] + before
            mine = owner_ids == owner[2 * c + h : 2 * c + h + 1]
            ranks.append(jnp.sum(jnp.where(mine, spot, 0.0), axis=0, keepdims=True))
        before = before + block[:, 2 * LANES :]
    ranking = jnp.concatenate(ranks, axis=0).astype(i32)
    code_ref[...] = owner * capacity_rows + (ranking >> 7)
    rank_ref[...] = ranking & (LANES - 1)

    lane_ids = iota((LANES, LANES), 0)
    steps = samp_rows // SUBLANES

    def place(t, placed):
        window = pl.ds(pl.multiple_of(t * SUBLANES, SUBLANES), SUBLANES)
        code, rank, low = code_ref[window], rank_ref[window], low_ref[window] + 1
        low_top = (low >> 8).astype(f32)
        low_rest = (low & 255).astype(f32)
        hot = jnp.concatenate([one_hot(code[r : r + 1], codes) for r in range(SUBLANES)], axis=1)
        tops, rests = [], []
        for r in range(SUBLANES):
            here = lane_ids == rank[r : r + 1]
            tops.append(jnp.where(here, low_top[r : r + 1], 0.0).astype(bf16))
            rests.append(jnp.where(here, low_rest[r : r + 1], 0.0).astype(bf16))
        values = jnp.concatenate(
            [jnp.concatenate(tops, axis=1), jnp.concatenate(rests, axis=1)], axis=0
        )
        return placed + lax.dot_general(
            hot, values, (((1,), (1,)), ((), ())), preferred_element_type=f32
        )

    placed = lax.fori_loop(0, steps, place, jnp.zeros((codes, 2 * LANES), f32))
    wanted = (placed[:, :LANES] * 256.0 + placed[:, LANES:]).astype(i32) - 1
    req_out[...] = cut(wanted, capacity_rows)

    all_of(0, amp_in).wait_recv()
    xr, xi = amp_in[:, 0], amp_in[:, 1]
    for bit in range(global_bits):
        xr, xi = leading_gate(xr, xi, bit, unit(local_bits + bit))
    weight = xr * xr + xi * xi
    wt_out[...] = weight
    scatter(2, wt_out, wt_in)

    @pl.loop(1, devices)
    def _(k):
        target = peer(k)
        ask(req_out.at[target], me, target).start()

    weight = join(weight)
    norm_part = jnp.sum(weight, axis=0, keepdims=True)
    low_depth = depth.bit_length() - 1
    code_shape = (rows, LANES)
    row_id = iota(code_shape, 0)
    row_value = (
        ((row_id >> low_depth) << local_bits)
        + (me << (7 + low_depth))
        + ((row_id & (depth - 1)) << 7)
    )
    lane_value = iota((LANES, LANES), 0)
    row_code = jnp.zeros(code_shape, i32)
    lane_code = jnp.zeros((LANES, LANES), i32)
    lane_mask = jnp.zeros((), i32)
    for k in range(marg_count):
        qubit = marg[0, k]
        row_code = row_code + (((row_value >> qubit) & 1) << k)
        lane_code = lane_code + (((lane_value >> qubit) & 1) << k)
        lane_mask = lane_mask + jnp.where(qubit < 7, 1 << k, 0)
    bins = 2**marg_count
    top, rest = halves(weight)
    split = jnp.concatenate([top, rest], axis=0)
    @pl.loop(0, bins // LANES)
    def _(c):
        bin_id = c * LANES + iota((1, LANES), 1)
        lane_part = bin_id & lane_mask
        lane_hot = (lane_code == lane_part).astype(f32).astype(bf16)
        folded = jnp.dot(split, lane_hot, preferred_element_type=f32)
        folded = folded[:rows] + folded[rows:]
        picked = jnp.where(row_code == bin_id - lane_part, folded, 0.0)
        his_out[0, pl.ds(c, 1)] = jnp.sum(picked, axis=0, keepdims=True)


    all_of(2, wt_in).wait_recv()
    spread(4, his_out, his_in)
    plain_ref[...] = join(wt_in[...])
    table_ref[...] = split_table(plain_ref[...])

    def parts(wanted):
        return wanted >> 7, wanted & (LANES - 1)

    def answers(wanted, other):
        found, second = lookup_both(
            table_ref[:, 0:rows], plain_ref, parts(wanted), parts(other)
        )
        return found, jnp.where(other >= 0, second, 0.0)

    def asked(k):
        source = peer(devices - k)
        ask(req_out.at[source], source, source).wait_recv()
        return source

    def send(source, found):
        ans_out[source] = found
        copy(3, ans_out.at[source], ans_in.at[me], source).start()

    source = asked(1)
    found, own = answers(req_in[source], req_out[me])
    send(source, found)
    ans_in[me] = own

    def reply(t, total):
        first, second = asked(2 * t), asked(2 * t + 1)
        found, other = answers(req_in[first], req_in[second])
        send(first, found)
        send(second, other)
        return total + jnp.sum(found + other, axis=0, keepdims=True)

    total = jnp.sum(found + own, axis=0, keepdims=True)
    total = lax.fori_loop(1, devices // 2, reply, total)
    tot_out[0, 0:1] = total
    tot_out[0, 1:2] = norm_part
    spread(5, tot_out, tot_in)

    all_of(3, ans_in).wait_recv()
    back_ref[...] = join(ans_in[...])
    table_ref[:, 0:codes] = split_table(back_ref[...])

    def fetch(t, carry):
        one = pl.ds(pl.multiple_of(2 * t * SUBLANES, SUBLANES), SUBLANES)
        two = pl.ds(pl.multiple_of((2 * t + 1) * SUBLANES, SUBLANES), SUBLANES)
        probs_ref[one], probs_ref[two] = lookup_both(
            table_ref[:, 0:codes],
            back_ref,
            (code_ref[one], rank_ref[one]),
            (code_ref[two], rank_ref[two]),
        )
        return carry

    lax.fori_loop(0, steps // 2, fetch, 0)
    all_of(5, tot_in).wait_recv()
    all_of(4, his_in).wait_recv()
    hist_ref[...] = jnp.sum(his_in[...], axis=0)
    fid_ref[...] = jnp.sum(tot_in[...], axis=0)

    for channel, into in enumerate((amp_in, req_in, wt_in, ans_in, his_in, tot_in)):
        all_of(channel, into).wait_send()


def finish(sizes, values, hist, totals, probs_ref, mine_ref, fid_ref):
    amps_total, samples = sizes
    bins, mine = float(hist.shape[0] * LANES), mine_ref.shape[1]
    start = lax.axis_index("dev") * mine
    sums = jnp.sum(totals[...], axis=1, keepdims=True)
    total, norm = sums[0:1], sums[1:2]
    probs_ref[...] = amps_total * (values[...] / norm)
    line = hist[pl.ds(start // LANES, 1)]
    line = jnp.broadcast_to(line, (SUBLANES, LANES))
    line = pltpu.roll(line, (LANES - start % LANES) % LANES, 1)
    mine_ref[...] = bins * (line[0:1, :mine] / norm)
    fid_ref[...] = amps_total * (total / norm) / samples - 1.0


def shards(state, angles, sample_high, sample_low, marginal_qubits):
    devices = lax.axis_size("dev")
    amps_local = state.shape[1]
    samp_local = sample_low.shape[0]
    marg_count = marginal_qubits.shape[0]
    bins = 2**marg_count
    depth = amps_local // devices // LANES
    capacity_rows = 4 * samp_local // devices // LANES
    rows = amps_local // LANES
    samp_rows = samp_local // LANES
    sizes = (
        devices,
        depth,
        capacity_rows,
        marg_count,
    )
    vmem = pl.BlockSpec(memory_space=pltpu.VMEM)
    smem = pl.BlockSpec(memory_space=pltpu.SMEM)
    codes = devices * capacity_rows
    bin_rows = bins // LANES
    values, hist, totals = pl.pallas_call(
        functools.partial(kernel, sizes),
        out_shape=(
            jax.ShapeDtypeStruct((samp_rows, LANES), f32),
            jax.ShapeDtypeStruct((bin_rows, LANES), f32),
            jax.ShapeDtypeStruct((2, LANES), f32),
        ),
        in_specs=[smem, smem, vmem, vmem, vmem],
        out_specs=(vmem, vmem, vmem),
        scratch_shapes=[
            pltpu.VMEM((devices, 2, depth, LANES), f32),
            pltpu.VMEM((devices, 2, depth, LANES), f32),
            pltpu.VMEM((devices, depth, LANES), f32),
            pltpu.VMEM((devices, depth, LANES), f32),
            pltpu.VMEM((devices, capacity_rows, LANES), i32),
            pltpu.VMEM((devices, capacity_rows, LANES), i32),
            pltpu.VMEM((devices, capacity_rows, LANES), f32),
            pltpu.VMEM((devices, capacity_rows, LANES), f32),
            pltpu.VMEM((1, bin_rows, LANES), f32),
            pltpu.VMEM((devices, bin_rows, LANES), f32),
            pltpu.VMEM((1, 2, LANES), f32),
            pltpu.VMEM((devices, 2, LANES), f32),
            pltpu.VMEM((samp_rows, LANES), i32),
            pltpu.VMEM((samp_rows, LANES), i32),
            pltpu.VMEM((2 * LANES, max(rows, codes)), bf16),
            pltpu.VMEM((rows, LANES), f32),
            pltpu.VMEM((codes, LANES), f32),
            pltpu.VMEM((8, -(-angles.shape[0] // SUBLANES) * SUBLANES, LANES), f32),
            pltpu.SemaphoreType.DMA((6,)),
            pltpu.SemaphoreType.DMA((6,)),
            pltpu.SemaphoreType.DMA((devices,)),
        ],
        compiler_params=pltpu.CompilerParams(collective_id=0, has_side_effects=True),
        name="circuit",
    )(
        angles.T,
        marginal_qubits.reshape(1, marg_count),
        state.reshape(2, rows, LANES).transpose(1, 0, 2).reshape(2 * rows, LANES),
        sample_high.reshape(samp_rows, LANES),
        sample_low.reshape(samp_rows, LANES),
    )
    probs, mine, fid = pl.pallas_call(
        functools.partial(finish, (float(amps_local * devices), float(samp_local * devices))),
        out_shape=(
            jax.ShapeDtypeStruct((samp_rows, LANES), f32),
            jax.ShapeDtypeStruct((1, bins // devices), f32),
            jax.ShapeDtypeStruct((1, 1), f32),
        ),
        in_specs=[vmem, vmem, vmem],
        out_specs=(vmem, vmem, vmem),
        name="finish",
    )(values, hist, totals)
    return probs.reshape(samp_local), mine.reshape(bins // devices), fid.reshape(())


def solution(mesh):
    return jax.shard_map(
        shards,
        mesh=mesh,
        in_specs=(P(None, "dev"), P(), P("dev", None), P("dev"), P()),
        out_specs=(P("dev"), P("dev"), P()),
        check_vma=False,
    )
```

```python
import functools

import jax
import jax.numpy as jnp
from jax import lax
from jax.experimental import pallas as pl
from jax.experimental.pallas import tpu as pltpu
from jax.sharding import PartitionSpec as P

LANES = 128
SUBLANES = 8
f32 = jnp.float32
bf16 = jnp.bfloat16
i32 = jnp.int32


def iota(shape, dim):
    return lax.broadcasted_iota(i32, shape, dim)


def gate_rows(angles, qubits):
    sub = iota((SUBLANES, LANES), 0)

    def column(j):
        blocks = []
        for first in range(0, qubits, SUBLANES):
            block = jnp.zeros((SUBLANES, LANES), f32)
            for q in range(first, min(first + SUBLANES, qubits)):
                block = jnp.where(sub == q - first, angles[j, q], block)
            blocks.append(block)
        return jnp.concatenate(blocks, axis=0)

    theta, first, second = column(0), column(1), column(2)
    cosine, sine = jnp.cos(theta), jnp.sin(theta)
    joint = first + second
    return [
        cosine,
        jnp.zeros_like(cosine),
        -jnp.cos(second) * sine,
        -jnp.sin(second) * sine,
        jnp.cos(first) * sine,
        jnp.sin(first) * sine,
        jnp.cos(joint) * cosine,
        jnp.sin(joint) * cosine,
    ]


def leading_gate(xr, xi, bit, u):
    n, s, lanes = xr.shape
    shape = (n >> (bit + 1), 2, 1 << bit, s, lanes)
    xr, xi = xr.reshape(shape), xi.reshape(shape)
    ar, ai, br, bi = xr[:, 0], xi[:, 0], xr[:, 1], xi[:, 1]
    outs_r, outs_i = [], []
    for row in range(2):
        pr, pi, qr, qi = u[4 * row : 4 * row + 4]
        outs_r.append(pr * ar - pi * ai + (qr * br - qi * bi))
        outs_i.append(pr * ai + pi * ar + (qr * bi + qi * br))
    return (
        jnp.stack(outs_r, 1).reshape(n, s, lanes),
        jnp.stack(outs_i, 1).reshape(n, s, lanes),
    )


def sublane_gate(xr, xi, bit, u):
    step = 1 << bit
    high = ((iota((SUBLANES, LANES), 0) >> bit) & 1) == 1

    def swap(x):
        down = pltpu.roll(x, step, 1)
        if 2 * step == SUBLANES:
            return down
        return jnp.where(high[None], down, pltpu.roll(x, SUBLANES - step, 1))

    keep_r = jnp.where(high, u[6], u[0])[None]
    keep_i = jnp.where(high, u[7], u[1])[None]
    cross_r = jnp.where(high, u[4], u[2])[None]
    cross_i = jnp.where(high, u[5], u[3])[None]
    yr, yi = swap(xr), swap(xi)
    return (
        keep_r * xr - keep_i * xi + (cross_r * yr - cross_i * yi),
        keep_r * xi + keep_i * xr + (cross_r * yi + cross_i * yr),
    )


def lane_matrix(units):
    shape = (LANES, LANES)
    row, col = iota(shape, 0), iota(shape, 1)
    mr = mi = None
    for bit, u in enumerate(units):
        rb, cb = ((row >> bit) & 1) == 1, ((col >> bit) & 1) == 1
        gr = jnp.where(cb, jnp.where(rb, u[6], u[4]), jnp.where(rb, u[2], u[0]))
        gi = jnp.where(cb, jnp.where(rb, u[7], u[5]), jnp.where(rb, u[3], u[1]))
        if mr is None:
            mr, mi = gr, gi
        else:
            mr, mi = mr * gr - mi * gi, mr * gi + mi * gr
    return mr, mi


def cut(x, depth):
    rows = x.shape[0]
    x = x.reshape(rows // SUBLANES, SUBLANES, LANES)
    per = SUBLANES // depth
    if per == 1:
        return x
    parts = [x[:, k * depth : (k + 1) * depth] for k in range(per)]
    return jnp.stack(parts, 1).reshape(rows // depth, depth, LANES)


def join(x):
    n, depth, _ = x.shape
    per = SUBLANES // depth
    if per > 1:
        x = x.reshape(n // per, per, depth, LANES)
        x = jnp.concatenate([x[:, k] for k in range(per)], axis=1)
    return x.reshape(n * depth, LANES)


def halves(x):
    top = x.astype(bf16)
    return top, (x - top.astype(f32)).astype(bf16)


def one_hot(row, count):
    wide = jnp.broadcast_to(row.astype(f32), (16, LANES)).astype(bf16)
    ids = iota((count, LANES), 0).astype(f32).astype(bf16).reshape(count // 16, 16, LANES)
    hot = jnp.where(ids == wide[None], jnp.ones((), bf16), jnp.zeros((), bf16))
    return hot.reshape(count, LANES)


def split_table(table):
    flipped = table.T
    top, rest = halves(flipped)
    return jnp.concatenate([top, rest], axis=0)


def lookup_dot(table, upper, lower):
    rows = upper.shape[0]
    count = table.shape[1]
    hot = jnp.concatenate([one_hot(upper[r : r + 1], count) for r in range(rows)], axis=1)
    both = jnp.dot(table, hot, preferred_element_type=f32)
    lane_ids = iota((LANES, LANES), 0)
    found = []
    for r in range(rows):
        part = slice(r * LANES, (r + 1) * LANES)
        value = both[:LANES, part] + both[LANES:, part]
        value = jnp.where(lane_ids == lower[r : r + 1], value, 0.0)
        found.append(jnp.sum(value, axis=0, keepdims=True))
    return jnp.concatenate(found, axis=0)


def lookup_lanes(table_ref, upper, lower):
    rows = upper.shape[0]
    if rows < SUBLANES:
        upper = jnp.concatenate([upper] * (SUBLANES // rows), axis=0)
        lower = jnp.concatenate([lower] * (SUBLANES // rows), axis=0)
    shape = (SUBLANES, LANES)
    bits = table_ref.shape[0].bit_length() - 1
    high = [((upper >> bit) & 1) == 1 for bit in range(bits)]

    def pick(first, bit):
        if bit < 0:
            line = jnp.broadcast_to(table_ref[first : first + 1], shape)
            return jnp.take_along_axis(line, lower, axis=1, mode="promise_in_bounds")
        zero = pick(first, bit - 1)
        return jnp.where(high[bit], pick(first + (1 << bit), bit - 1), zero)

    return pick(0, bits - 1)[:rows]


def lookup_both(table, plain, wanted, other):
    one = lookup_dot(table, wanted[0], wanted[1])
    return one, lookup_lanes(plain, other[0], other[1])


def kernel(
    sizes,
    angles,
    marg,
    state,
    owner_ref,
    low_ref,
    probs_ref,
    hist_ref,
    fid_ref,
    amp_out,
    amp_in,
    wt_out,
    wt_in,
    req_out,
    req_in,
    ans_out,
    ans_in,
    his_out,
    his_in,
    tot_out,
    tot_in,
    code_ref,
    rank_ref,
    table_ref,
    plain_ref,
    back_ref,
    gates,
    sends,
    recvs,
    req_recvs,
):
    devices, depth, capacity_rows, marg_count = sizes
    me = lax.axis_index("dev")
    global_bits = devices.bit_length() - 1
    rows = state.shape[0] // 2
    row_bits = rows.bit_length() - 1
    local_bits = row_bits + 7
    codes = devices * capacity_rows

    def peer(k):
        return lax.rem(me + k, devices)

    def copy(channel, src, dst, target):
        return pltpu.make_async_remote_copy(
            src_ref=src,
            dst_ref=dst,
            send_sem=sends.at[channel],
            recv_sem=recvs.at[channel],
            device_id=(target,),
            device_id_type=pl.DeviceIdType.MESH,
        )

    def scatter(channel, out, into):
        @pl.loop(1, devices)
        def _(k):
            target = peer(1 + lax.rem(k + devices // 3, devices - 1))
            copy(channel, out.at[target], into.at[me], target).start()

        into[me] = out[me]

    def spread(channel, out, into):
        @pl.loop(1, devices)
        def _(k):
            copy(channel, out.at[0], into.at[me], peer(k)).start()

        into[me] = out[0]

    def all_of(channel, into):
        many = into.at[pl.ds(0, devices - 1)]
        return copy(channel, many, many, peer(1))

    def ask(src, source, target):
        return pltpu.make_async_remote_copy(
            src_ref=src,
            dst_ref=req_in.at[source],
            send_sem=sends.at[1],
            recv_sem=req_recvs.at[source],
            device_id=(target,),
            device_id_type=pl.DeviceIdType.MESH,
        )

    barrier = pltpu.get_barrier_semaphore()

    @pl.loop(1, devices)
    def _(k):
        pl.semaphore_signal(
            barrier, inc=1, device_id=(peer(k),), device_id_type=pl.DeviceIdType.MESH
        )

    for e, entry in enumerate(gate_rows(angles, global_bits + local_bits)):
        gates[e] = entry

    def unit(qubit):
        return [gates[e, qubit : qubit + 1] for e in range(8)]

    mr, mi = lane_matrix([unit(q) for q in range(7)])
    mixed = jnp.concatenate(
        [jnp.concatenate([mr, mi], axis=1), jnp.concatenate([-mi, mr], axis=1)], axis=0
    )
    both = jnp.concatenate(
        [state[pl.ds(0, rows, stride=2)], state[pl.ds(1, rows, stride=2)]], axis=1
    )
    both = jnp.dot(both, mixed, precision=lax.Precision.HIGHEST, preferred_element_type=f32)
    xr = both[:, :LANES].reshape(rows // SUBLANES, SUBLANES, LANES)
    xi = both[:, LANES:].reshape(rows // SUBLANES, SUBLANES, LANES)
    for bit in range(3):
        xr, xi = sublane_gate(xr, xi, bit, unit(7 + bit))
    for bit in range(row_bits - 3):
        xr, xi = leading_gate(xr, xi, bit, unit(10 + bit))
    amp_out[:, 0] = cut(xr.reshape(rows, LANES), depth)
    amp_out[:, 1] = cut(xi.reshape(rows, LANES), depth)

    pl.semaphore_wait(barrier, devices - 1)
    scatter(0, amp_out, amp_in)

    samp_rows = owner_ref.shape[0]
    owner = owner_ref[...]
    owner_ids = iota((devices, LANES), 0)
    chunks = samp_rows // 2
    hot_rows = [(owner_ids == owner[r : r + 1]) for r in range(samp_rows)]
    pieces = [h.astype(f32).astype(bf16) for h in hot_rows]
    stacked = jnp.concatenate(
        [jnp.concatenate(pieces[2 * c : 2 * c + 2], axis=1) for c in range(chunks)], axis=0
    )
    tri_shape = (2 * LANES, 3 * LANES)
    tri_row, tri_col = iota(tri_shape, 0), iota(tri_shape, 1)
    tri = ((tri_row < tri_col) | (tri_col >= 2 * LANES)).astype(f32).astype(bf16)
    counts = jnp.dot(stacked, tri, preferred_element_type=f32)
    before = jnp.zeros((devices, LANES), f32)
    ranks = []
    for c in range(chunks):
        block = counts[c * devices : (c + 1) * devices]
        for h in range(2):
            spot = block[:, h * LANES : (h + 1) * LANES] + before
            mine = owner_ids == owner[2 * c + h : 2 * c + h + 1]
            ranks.append(jnp.sum(jnp.where(mine, spot, 0.0), axis=0, keepdims=True))
        before = before + block[:, 2 * LANES :]
    ranking = jnp.concatenate(ranks, axis=0).astype(i32)
    code_ref[...] = owner * capacity_rows + (ranking >> 7)
    rank_ref[...] = ranking & (LANES - 1)

    lane_ids = iota((LANES, LANES), 0)
    steps = samp_rows // SUBLANES

    def place(t, placed):
        window = pl.ds(pl.multiple_of(t * SUBLANES, SUBLANES), SUBLANES)
        code, rank, low = code_ref[window], rank_ref[window], low_ref[window] + 1
        low_top = (low >> 8).astype(f32)
        low_rest = (low & 255).astype(f32)
        hot = jnp.concatenate([one_hot(code[r : r + 1], codes) for r in range(SUBLANES)], axis=1)
        tops, rests = [], []
        for r in range(SUBLANES):
            here = lane_ids == rank[r : r + 1]
            tops.append(jnp.where(here, low_top[r : r + 1], 0.0).astype(bf16))
            rests.append(jnp.where(here, low_rest[r : r + 1], 0.0).astype(bf16))
        values = jnp.concatenate(
            [jnp.concatenate(tops, axis=1), jnp.concatenate(rests, axis=1)], axis=0
        )
        return placed + lax.dot_general(
            hot, values, (((1,), (1,)), ((), ())), preferred_element_type=f32
        )

    placed = lax.fori_loop(0, steps, place, jnp.zeros((codes, 2 * LANES), f32))
    wanted = (placed[:, :LANES] * 256.0 + placed[:, LANES:]).astype(i32) - 1
    req_out[...] = cut(wanted, capacity_rows)

    all_of(0, amp_in).wait_recv()
    xr, xi = amp_in[:, 0], amp_in[:, 1]
    for bit in range(global_bits):
        xr, xi = leading_gate(xr, xi, bit, unit(local_bits + bit))
    weight = xr * xr + xi * xi
    wt_out[...] = weight
    scatter(2, wt_out, wt_in)

    weight = join(weight)
    norm_part = jnp.sum(weight, axis=0, keepdims=True)
    low_depth = depth.bit_length() - 1
    code_shape = (rows, LANES)
    row_id = iota(code_shape, 0)
    row_value = (
        ((row_id >> low_depth) << local_bits)
        + (me << (7 + low_depth))
        + ((row_id & (depth - 1)) << 7)
    )
    lane_value = iota((LANES, LANES), 0)
    row_code = jnp.zeros(code_shape, i32)
    lane_code = jnp.zeros((LANES, LANES), i32)
    lane_mask = jnp.zeros((), i32)
    for k in range(marg_count):
        qubit = marg[0, k]
        row_code = row_code + (((row_value >> qubit) & 1) << k)
        lane_code = lane_code + (((lane_value >> qubit) & 1) << k)
        lane_mask = lane_mask + jnp.where(qubit < 7, 1 << k, 0)
    bins = 2**marg_count
    top, rest = halves(weight)
    split = jnp.concatenate([top, rest], axis=0)
    @pl.loop(0, bins // LANES)
    def _(c):
        bin_id = c * LANES + iota((1, LANES), 1)
        lane_part = bin_id & lane_mask
        lane_hot = (lane_code == lane_part).astype(f32).astype(bf16)
        folded = jnp.dot(split, lane_hot, preferred_element_type=f32)
        folded = folded[:rows] + folded[rows:]
        picked = jnp.where(row_code == bin_id - lane_part, folded, 0.0)
        his_out[0, pl.ds(c, 1)] = jnp.sum(picked, axis=0, keepdims=True)


    @pl.loop(1, devices)
    def _(k):
        target = peer(k)
        ask(req_out.at[target], me, target).start()

    all_of(2, wt_in).wait_recv()
    spread(4, his_out, his_in)
    plain_ref[...] = join(wt_in[...])
    table_ref[...] = split_table(plain_ref[...])

    def parts(wanted):
        return wanted >> 7, wanted & (LANES - 1)

    def answers(wanted, other):
        found, second = lookup_both(
            table_ref[:, 0:rows], plain_ref, parts(wanted), parts(other)
        )
        return found, jnp.where(other >= 0, second, 0.0)

    def asked(k):
        source = peer(devices - k)
        ask(req_out.at[source], source, source).wait_recv()
        return source

    def send(source, found):
        ans_out[source] = found
        copy(3, ans_out.at[source], ans_in.at[me], source).start()

    source = asked(1)
    found, own = answers(req_in[source], req_out[me])
    send(source, found)
    ans_in[me] = own

    def reply(t, total):
        first, second = asked(2 * t), asked(2 * t + 1)
        found, other = answers(req_in[first], req_in[second])
        send(first, found)
        send(second, other)
        return total + jnp.sum(found + other, axis=0, keepdims=True)

    total = jnp.sum(found + own, axis=0, keepdims=True)
    total = lax.fori_loop(1, devices // 2, reply, total)
    tot_out[0, 0:1] = total
    tot_out[0, 1:2] = norm_part
    spread(5, tot_out, tot_in)

    all_of(3, ans_in).wait_recv()
    back_ref[...] = join(ans_in[...])
    table_ref[:, 0:codes] = split_table(back_ref[...])

    def fetch(t, carry):
        one = pl.ds(pl.multiple_of(2 * t * SUBLANES, SUBLANES), SUBLANES)
        two = pl.ds(pl.multiple_of((2 * t + 1) * SUBLANES, SUBLANES), SUBLANES)
        probs_ref[one], probs_ref[two] = lookup_both(
            table_ref[:, 0:codes],
            back_ref,
            (code_ref[one], rank_ref[one]),
            (code_ref[two], rank_ref[two]),
        )
        return carry

    lax.fori_loop(0, steps // 2, fetch, 0)
    all_of(5, tot_in).wait_recv()
    all_of(4, his_in).wait_recv()
    hist_ref[...] = jnp.sum(his_in[...], axis=0)
    fid_ref[...] = jnp.sum(tot_in[...], axis=0)

    for channel, into in enumerate((amp_in, req_in, wt_in, ans_in, his_in, tot_in)):
        all_of(channel, into).wait_send()


def finish(sizes, values, hist, totals, probs_ref, mine_ref, fid_ref):
    amps_total, samples = sizes
    bins, mine = float(hist.shape[0] * LANES), mine_ref.shape[1]
    start = lax.axis_index("dev") * mine
    sums = jnp.sum(totals[...], axis=1, keepdims=True)
    total, norm = sums[0:1], sums[1:2]
    probs_ref[...] = amps_total * (values[...] / norm)
    line = hist[pl.ds(start // LANES, 1)]
    line = jnp.broadcast_to(line, (SUBLANES, LANES))
    line = pltpu.roll(line, (LANES - start % LANES) % LANES, 1)
    mine_ref[...] = bins * (line[0:1, :mine] / norm)
    fid_ref[...] = amps_total * (total / norm) / samples - 1.0


def shards(state, angles, sample_high, sample_low, marginal_qubits):
    devices = lax.axis_size("dev")
    amps_local = state.shape[1]
    samp_local = sample_low.shape[0]
    marg_count = marginal_qubits.shape[0]
    bins = 2**marg_count
    depth = amps_local // devices // LANES
    capacity_rows = 4 * samp_local // devices // LANES
    rows = amps_local // LANES
    samp_rows = samp_local // LANES
    sizes = (
        devices,
        depth,
        capacity_rows,
        marg_count,
    )
    vmem = pl.BlockSpec(memory_space=pltpu.VMEM)
    smem = pl.BlockSpec(memory_space=pltpu.SMEM)
    codes = devices * capacity_rows
    bin_rows = bins // LANES
    values, hist, totals = pl.pallas_call(
        functools.partial(kernel, sizes),
        out_shape=(
            jax.ShapeDtypeStruct((samp_rows, LANES), f32),
            jax.ShapeDtypeStruct((bin_rows, LANES), f32),
            jax.ShapeDtypeStruct((2, LANES), f32),
        ),
        in_specs=[smem, smem, vmem, vmem, vmem],
        out_specs=(vmem, vmem, vmem),
        scratch_shapes=[
            pltpu.VMEM((devices, 2, depth, LANES), f32),
            pltpu.VMEM((devices, 2, depth, LANES), f32),
            pltpu.VMEM((devices, depth, LANES), f32),
            pltpu.VMEM((devices, depth, LANES), f32),
            pltpu.VMEM((devices, capacity_rows, LANES), i32),
            pltpu.VMEM((devices, capacity_rows, LANES), i32),
            pltpu.VMEM((devices, capacity_rows, LANES), f32),
            pltpu.VMEM((devices, capacity_rows, LANES), f32),
            pltpu.VMEM((1, bin_rows, LANES), f32),
            pltpu.VMEM((devices, bin_rows, LANES), f32),
            pltpu.VMEM((1, 2, LANES), f32),
            pltpu.VMEM((devices, 2, LANES), f32),
            pltpu.VMEM((samp_rows, LANES), i32),
            pltpu.VMEM((samp_rows, LANES), i32),
            pltpu.VMEM((2 * LANES, max(rows, codes)), bf16),
            pltpu.VMEM((rows, LANES), f32),
            pltpu.VMEM((codes, LANES), f32),
            pltpu.VMEM((8, -(-angles.shape[0] // SUBLANES) * SUBLANES, LANES), f32),
            pltpu.SemaphoreType.DMA((6,)),
            pltpu.SemaphoreType.DMA((6,)),
            pltpu.SemaphoreType.DMA((devices,)),
        ],
        compiler_params=pltpu.CompilerParams(collective_id=0, has_side_effects=True),
        name="circuit",
    )(
        angles.T,
        marginal_qubits.reshape(1, marg_count),
        state.reshape(2, rows, LANES).transpose(1, 0, 2).reshape(2 * rows, LANES),
        sample_high.reshape(samp_rows, LANES),
        sample_low.reshape(samp_rows, LANES),
    )
    probs, mine, fid = pl.pallas_call(
        functools.partial(finish, (float(amps_local * devices), float(samp_local * devices))),
        out_shape=(
            jax.ShapeDtypeStruct((samp_rows, LANES), f32),
            jax.ShapeDtypeStruct((1, bins // devices), f32),
            jax.ShapeDtypeStruct((1, 1), f32),
        ),
        in_specs=[vmem, vmem, vmem],
        out_specs=(vmem, vmem, vmem),
        name="finish",
    )(values, hist, totals)
    return probs.reshape(samp_local), mine.reshape(bins // devices), fid.reshape(())


def solution(mesh):
    return jax.shard_map(
        shards,
        mesh=mesh,
        in_specs=(P(None, "dev"), P(), P("dev", None), P("dev"), P()),
        out_specs=(P("dev"), P("dev"), P()),
        check_vma=False,
    )
```
